32 devices in a mesh: dp: 1 (over z), tp: 4 (over y), sp: 8 (over x, core).
Axes of the slice: x: 4, y: 4, z: 1, core: 2. Of those that a mesh axis runs over, the one named last changes fastest.
The devices are a block of a 4x4x8 slice.
Arguments:
- hidden: bfloat16 [16, 4096], P('dp')
- k_cache: bfloat16 [16, 4096, 32, 128], P('dp', 'sp', 'tp')
- v_cache: bfloat16 [16, 4096, 32, 128], P('dp', 'sp', 'tp')
- lengths: int32 [16], P('dp')
- rel_table: bfloat16 [4096, 32, 128], P('sp', 'tp')
- u_bias: bfloat16 [32, 128], P('tp')
- w_bias: bfloat16 [32, 128], P('tp')
- g_attn: bfloat16 [4096], replicated
- w_query: bfloat16 [4096, 32, 128], P(None, 'tp')
- w_key: bfloat16 [4096, 32, 128], P(None, 'tp')
- w_value: bfloat16 [4096, 32, 128], P(None, 'tp')
- w_out: bfloat16 [32, 128, 4096], P('tp')
- g_mlp: bfloat16 [4096], replicated
- w_up: bfloat16 [4096, 16384], P(None, 'tp')
- w_down: bfloat16 [16384, 4096], P('tp')
Outputs:
- output: bfloat16 [16, 4096], P('dp')
All inputs are finite; a program needn't handle non-finite values.
Results may differ from the reference program's by a relative error of at most 0.014473.
Values sent between devices are 32-bit elements.
A program may use at most 768 MiB of HBM per device.

```python
import math
import jax
import jax.numpy as jnp
from jax import lax

BATCH = 16
SMAX = 4096
D = 4096
HEADS = 32
HEAD = 128
FF = 16384
EPS = 1e-6
MASKED = -1e30


def setup_inputs(seed: int = 0, part: int = 0) -> dict:
    base = jax.random.key(seed)
    shared_keys = jax.random.split(base, 11)
    part_keys = jax.random.split(jax.random.fold_in(base, part), 5)
    key_scale = math.sqrt(math.log(SMAX / 32.0) / 4.0)
    cache_shape = (BATCH, SMAX, HEADS, HEAD)
    hidden = jax.random.normal(part_keys[0], (BATCH, D), jnp.float32)
    k_cache = jax.random.normal(part_keys[1], cache_shape, jnp.float32) * key_scale
    v_cache = jax.random.normal(part_keys[2], cache_shape, jnp.float32)
    drawn_len = jax.random.randint(part_keys[3], (BATCH,), SMAX // 8, SMAX)
    full_slot = jax.random.randint(part_keys[4], (), 0, BATCH)
    lengths = jnp.where(jnp.arange(BATCH) == full_slot, SMAX - 1, drawn_len).astype(jnp.int32)
    rel_table = jax.random.normal(shared_keys[0], (SMAX, HEADS, HEAD), jnp.float32) * key_scale
    u_bias = jax.random.normal(shared_keys[1], (HEADS, HEAD), jnp.float32)
    w_bias = jax.random.normal(shared_keys[2], (HEADS, HEAD), jnp.float32)
    g_attn = 1.0 + 0.3 * jax.random.normal(shared_keys[3], (D,), jnp.float32)
    w_query = jax.random.normal(shared_keys[4], (D, HEADS, HEAD), jnp.float32) * D ** -0.5
    w_key = jax.random.normal(shared_keys[5], (D, HEADS, HEAD), jnp.float32) * (2.5 * key_scale * D ** -0.5)
    w_value = jax.random.normal(shared_keys[6], (D, HEADS, HEAD), jnp.float32) * (2.0 * D ** -0.5)
    w_out = jax.random.normal(shared_keys[7], (HEADS, HEAD, D), jnp.float32) * (3.0 * (HEADS * HEAD) ** -0.5)
    g_mlp = 1.0 + 0.3 * jax.random.normal(shared_keys[8], (D,), jnp.float32)
    w_up = jax.random.normal(shared_keys[9], (D, FF), jnp.float32) * D ** -0.5
    w_down = jax.random.normal(shared_keys[10], (FF, D), jnp.float32) * FF ** -0.5
    return {
        'hidden': hidden.astype(jnp.bfloat16),
        'k_cache': k_cache.astype(jnp.bfloat16),
        'v_cache': v_cache.astype(jnp.bfloat16),
        'lengths': lengths,
        'rel_table': rel_table.astype(jnp.bfloat16),
        'u_bias': u_bias.astype(jnp.bfloat16),
        'w_bias': w_bias.astype(jnp.bfloat16),
        'g_attn': g_attn.astype(jnp.bfloat16),
        'w_query': w_query.astype(jnp.bfloat16),
        'w_key': w_key.astype(jnp.bfloat16),
        'w_value': w_value.astype(jnp.bfloat16),
        'w_out': w_out.astype(jnp.bfloat16),
        'g_mlp': g_mlp.astype(jnp.bfloat16),
        'w_up': w_up.astype(jnp.bfloat16),
        'w_down': w_down.astype(jnp.bfloat16),
    }


def rms_norm(tensor, gain):
    wide = tensor.astype(jnp.float32)
    mean_sq = jnp.mean(wide * wide, axis=-1, keepdims=True)
    return (wide * lax.rsqrt(mean_sq + EPS) * gain.astype(jnp.float32)).astype(jnp.bfloat16)


def reference(hidden, k_cache, v_cache, lengths, rel_table, u_bias, w_bias, g_attn, w_query, w_key, w_value, w_out, g_mlp, w_up, w_down):
    normed = rms_norm(hidden, g_attn)
    query_vec = jnp.dot(normed, w_query.reshape(D, HEADS * HEAD), preferred_element_type=jnp.float32).astype(jnp.bfloat16).reshape(BATCH, HEADS, HEAD)
    key_new = jnp.dot(normed, w_key.reshape(D, HEADS * HEAD), preferred_element_type=jnp.float32).astype(jnp.bfloat16).reshape(BATCH, HEADS, HEAD)
    value_new = jnp.dot(normed, w_value.reshape(D, HEADS * HEAD), preferred_element_type=jnp.float32).astype(jnp.bfloat16).reshape(BATCH, HEADS, HEAD)
    positions = jnp.arange(SMAX)
    write_mask = (positions[None, :] == lengths[:, None])[:, :, None, None]
    k_updated = jnp.where(write_mask, key_new[:, None], k_cache)
    v_updated = jnp.where(write_mask, value_new[:, None], v_cache)
    q_content = (query_vec.astype(jnp.float32) + u_bias.astype(jnp.float32)).astype(jnp.bfloat16)
    q_position = (query_vec.astype(jnp.float32) + w_bias.astype(jnp.float32)).astype(jnp.bfloat16)
    rel_wide = rel_table.astype(jnp.float32)

    def attend_one(packed):
        q_cont, q_pos, k_seq, v_seq, length = packed
        content = jnp.einsum('hd,shd->hs', q_cont.astype(jnp.float32), k_seq.astype(jnp.float32))
        by_distance = jnp.einsum('hd,shd->hs', q_pos.astype(jnp.float32), rel_wide)
        distance = length - positions
        relative = by_distance[:, jnp.clip(distance, 0, SMAX - 1)]
        scores = (content + relative) * (HEAD ** -0.5)
        scores = jnp.where((distance >= 0)[None, :], scores, MASKED)
        weights = jax.nn.softmax(scores, axis=-1)
        return jnp.einsum('hs,shd->hd', weights, v_seq.astype(jnp.float32)).astype(jnp.bfloat16)

    context = lax.map(attend_one, (q_content, q_position, k_updated, v_updated, lengths))
    attn_out = jnp.dot(context.reshape(BATCH, HEADS * HEAD), w_out.reshape(HEADS * HEAD, D), preferred_element_type=jnp.float32)
    resid_mid = (hidden.astype(jnp.float32) + attn_out).astype(jnp.bfloat16)
    normed_mlp = rms_norm(resid_mid, g_mlp)
    up_proj = jnp.dot(normed_mlp, w_up, preferred_element_type=jnp.float32)
    activated = jax.nn.gelu(up_proj, approximate=True).astype(jnp.bfloat16)
    down_proj = jnp.dot(activated, w_down, preferred_element_type=jnp.float32)
    hidden_out = (resid_mid.astype(jnp.float32) + down_proj).astype(jnp.bfloat16)
    return hidden_out
```

```python
import functools

import jax
import jax.numpy as jnp
from jax import lax
from jax.experimental import pallas as pl
from jax.experimental.pallas import tpu as pltpu
from jax.sharding import PartitionSpec as P

EPS = 1e-6
MASKED = -1e30
FLOOR = -5e29
LANES = 128
F32 = jnp.float32
BF16 = jnp.bfloat16
NT = (((1,), (1,)), ((), ()))


def layer_kernel(n_sp, n_tp,
                 lens, hid, u_ref, w_ref, ga, gm, rel_hbm, k_hbm, v_hbm, wq_hbm, wk_hbm, wv_hbm, wo_hbm, wu_hbm, wd_hbm,
                 out_ref,
                 wqkv, relb, rrev, kb, vb, wob, wub, wdb,
                 qsend, qrecv, kvsend, kvrecv, qall, qcb, relsend, grid_rel, win, sc, csend, crecv, call, aosend, aorecv,
                 x1all, aall, dnsend, dnrecv, oall,
                 hsem, ssem, rsem, rel_ssem, rel_rsem, tp_ssem, tp_rsem):
    me = lax.axis_index('sp')
    my_tp = lax.axis_index('tp')
    batch = hid.shape[0]
    heads = u_ref.shape[0]
    head_dim = u_ref.shape[1]
    rows = kb.shape[1]
    seq_blk = rows // heads
    kk = wqkv.shape[1] // heads
    co = wob.shape[1]
    per_row = LANES // heads
    rel_rows = seq_blk // per_row
    smax = seq_blk * n_sp
    half = rows // 2
    scale = head_dim ** -0.5

    copies = []

    def fetch(src, dst):
        copy = pltpu.make_async_copy(src, dst, hsem.at[len(copies)])
        copies.append(copy)
        copy.start()
        return copy

    w_rows = pl.ds(pl.multiple_of(me * kk * heads, kk * heads), kk * heads)
    w_copies = [fetch(src.at[w_rows], wqkv.at[i]) for i, src in enumerate((wq_hbm, wk_hbm, wv_hbm))]
    rel_copy = fetch(rel_hbm, relb)
    k_copies = [fetch(k_hbm.at[b], kb.at[b]) for b in range(batch)]
    v_copies = [fetch(v_hbm.at[b], vb.at[b]) for b in range(batch)]
    o_cols = pl.ds(pl.multiple_of(me * co, co), co)
    wo_copy = fetch(wo_hbm.at[:, o_cols], wob)
    f_cols = pl.ds(pl.multiple_of(me * wub.shape[1], wub.shape[1]), wub.shape[1])
    wu_copy = fetch(wu_hbm.at[:, f_cols], wub)
    wd_copy = fetch(wd_hbm.at[:, o_cols], wdb)

    def sp_peer(off):
        return lax.rem(me + off, n_sp)

    def tp_peer(off):
        return lax.rem(my_tp + off, n_tp)

    grid_rel[...] = jnp.zeros_like(grid_rel)

    barrier = pltpu.get_barrier_semaphore()
    for off in range(1, n_sp):
        pl.semaphore_signal(barrier, inc=1, device_id={'sp': sp_peer(off)}, device_id_type=pl.DeviceIdType.MESH)
    for off in range(1, n_tp):
        pl.semaphore_signal(barrier, inc=1, device_id={'tp': tp_peer(off)}, device_id_type=pl.DeviceIdType.MESH)

    def remote(src, dst, send, recv, where):
        return pltpu.make_async_remote_copy(src_ref=src, dst_ref=dst, send_sem=send, recv_sem=recv, device_id=where,
                                            device_id_type=pl.DeviceIdType.MESH)

    sends = []

    def scatter(phase, src, dst):
        for off in range(1, n_sp):
            peer = sp_peer(off)
            copy = remote(src.at[peer], dst.at[me], ssem.at[phase, peer], rsem.at[phase, me], {'sp': peer})
            copy.start()
            sends.append(copy)

    def gather(phase, buf):
        for off in range(1, n_sp):
            peer = sp_peer(off)
            copy = remote(buf.at[me], buf.at[me], ssem.at[phase, peer], rsem.at[phase, me], {'sp': peer})
            copy.start()
            sends.append(copy)

    def arrived(phase, buf):
        for off in range(1, n_sp):
            peer = sp_peer(off)
            remote(buf.at[peer], buf.at[peer], ssem.at[phase, peer], rsem.at[phase, peer], {'sp': peer}).wait_recv()

    def tp_sum(phase, src, dst):
        dst[my_tp] = src[...]
        for off in range(1, n_tp):
            peer = tp_peer(off)
            copy = remote(src, dst.at[my_tp], tp_ssem.at[phase, peer], tp_rsem.at[phase, my_tp], {'tp': peer})
            copy.start()
            sends.append(copy)
        for off in range(1, n_tp):
            peer = tp_peer(off)
            remote(src, dst.at[peer], tp_ssem.at[phase, peer], tp_rsem.at[phase, peer], {'tp': peer}).wait_recv()
        total = dst[0]
        for t in range(1, n_tp):
            total = total + dst[t]
        return total

    wide = hid[...].astype(F32)
    inv = lax.rsqrt(jnp.mean(wide * wide, axis=-1, keepdims=True) + EPS)
    k_cols = pl.ds(pl.multiple_of(me * kk, kk), kk)
    normed = (hid[:, k_cols].astype(F32) * inv * ga[:, k_cols].astype(F32)).astype(BF16)

    spread = (lax.broadcasted_iota(jnp.int32, (LANES, LANES * heads), 1) // heads
              == lax.broadcasted_iota(jnp.int32, (LANES, LANES * heads), 0)).astype(F32).astype(BF16)
    wide_lane_head = lax.broadcasted_iota(jnp.int32, (batch, LANES * heads), 1) % heads
    lhs = []
    for c in range(kk // LANES):
        spread_in = jnp.dot(normed[:, c * LANES:(c + 1) * LANES], spread, preferred_element_type=F32)
        lhs.append(jnp.concatenate([jnp.where(wide_lane_head == h, spread_in, 0.0).astype(BF16) for h in range(heads)], axis=0))
    parts = []
    for i in range(3):
        w_copies[i].wait()
        acc = jnp.zeros((heads * batch, head_dim), F32)
        for c in range(kk // LANES):
            span = LANES * heads
            acc = acc + jnp.dot(lhs[c], wqkv[i, c * span:(c + 1) * span, :], preferred_element_type=F32)
        if i == 0:
            for h in range(heads):
                qsend[h] = acc[h * batch:(h + 1) * batch]
            pl.semaphore_wait(barrier, n_sp + n_tp - 2)
            scatter(0, qsend, qrecv)
            qrecv[me] = qsend[me]
        else:
            for h in range(heads):
                kvsend[h, i - 1] = acc[h * batch:(h + 1) * batch]
    scatter(1, kvsend, kvrecv)
    kvrecv[me] = kvsend[me]

    rel_copy.wait()
    group = 32

    def reverse(i, carry):
        tile = relb[pl.ds(pl.multiple_of(i * group, group), group)].astype(F32)
        flipped = jnp.concatenate([tile[group - 1 - j:group - j] for j in range(group)], axis=0)
        flipped = flipped.reshape(group * heads, head_dim).astype(BF16)
        at = pl.multiple_of((seq_blk // group - 1 - i) * group * heads, group * heads)
        rrev[pl.ds(at, group * heads), :] = flipped
        return carry

    lax.fori_loop(0, seq_blk // group, reverse, 0)

    arrived(0, qrecv)
    q_head = qrecv[0]
    for p in range(1, n_sp):
        q_head = q_head + qrecv[p]
    qall[me] = q_head.astype(BF16).astype(F32)
    gather(2, qall)
    arrived(2, qall)

    u_wide, w_wide = u_ref[...].astype(F32), w_ref[...].astype(F32)
    q_pos = jnp.concatenate([(qall[h] + w_wide[h:h + 1]).astype(BF16) for h in range(heads)], axis=0)
    lane_head = lax.broadcasted_iota(jnp.int32, (batch, LANES), 1) % heads

    def relative(c, carry):
        span = 2 * LANES
        table = rrev[pl.ds(pl.multiple_of(c * span, span), span), :]
        by_head = lax.dot_general(q_pos, table, NT, preferred_element_type=F32)
        for t in range(2):
            tile = by_head[:, t * LANES:(t + 1) * LANES]
            row = tile[:batch]
            for h in range(1, heads):
                row = jnp.where(lane_head == h, tile[h * batch:(h + 1) * batch], row)
            relsend[:, pl.ds(2 * c + t, 1), :] = row.reshape(batch, 1, LANES)
        return carry

    lax.fori_loop(0, rows // (2 * LANES), relative, 0)

    def rel_slot(src, dst):
        return grid_rel.at[:, pl.ds(pl.multiple_of((n_sp - 1 - src - dst) * rel_rows, rel_rows), rel_rows), :]

    for off in range(1, n_sp):
        peer = sp_peer(off)

        @pl.when(peer + me <= n_sp - 1)
        def _():
            remote(relsend, rel_slot(me, peer), rel_ssem.at[peer], rel_rsem.at[me], {'sp': peer}).start()

    @pl.when(me + me <= n_sp - 1)
    def _():
        at = pl.multiple_of((n_sp - 1 - me - me) * rel_rows, rel_rows)
        grid_rel[:, pl.ds(at, rel_rows), :] = relsend[...]

    for h in range(heads):
        qcb[:, h:h + 1, :] = (qall[h] + u_wide[h:h + 1]).reshape(batch, 1, head_dim)

    def wait_for(copy_src, copy_dst, b, first):
        pltpu.make_async_copy(copy_src.at[b], copy_dst.at[b], hsem.at[first + b]).wait()

    def content(b, carry):
        wait_for(k_hbm, kb, b, 4)
        q = qcb[b]
        zero = jnp.zeros_like(q)
        two = jnp.concatenate([jnp.concatenate([q, zero], axis=1), jnp.concatenate([zero, q], axis=1)], axis=0).astype(BF16)
        for c in range(half // 256):
            keys = jnp.concatenate([kb[b, c * 256:(c + 1) * 256, :], kb[b, half + c * 256:half + (c + 1) * 256, :]], axis=1)
            sc[b, :, c * 256:(c + 1) * 256] = lax.dot_general(two, keys, NT, preferred_element_type=F32)
        return carry

    lax.fori_loop(0, batch, content, 0)

    for off in range(1, n_sp):
        peer = sp_peer(off)

        @pl.when(peer + me <= n_sp - 1)
        def _():
            remote(relsend, rel_slot(peer, me), rel_ssem.at[peer], rel_rsem.at[peer], {'sp': peer}).wait_recv()

    r_iota = lax.broadcasted_iota(jnp.int32, (2 * heads, LANES), 0)
    l_iota = lax.broadcasted_iota(jnp.int32, (2 * heads, LANES), 1)
    slot = me * seq_blk + (r_iota // heads) * (seq_blk // 2) + l_iota // heads
    slot = jnp.where(r_iota % heads == l_iota % heads, slot, jnp.int32(2 ** 30))
    lane_row = lax.broadcasted_iota(jnp.int32, (rel_rows, LANES), 1)
    first_stat = lax.broadcasted_iota(jnp.int32, (heads, LANES), 1) < LANES // 2
    tiles = half // LANES

    def attend(b, carry):
        n = lens[b]
        start = smax - 1 - n
        row0 = jnp.minimum(start // per_row, (n_sp - 1) * rel_rows)
        turn = LANES - heads * (start % per_row)
        now = pltpu.roll(grid_rel[b, pl.ds(row0, rel_rows), :], turn, 1)
        after = pltpu.roll(grid_rel[b, pl.ds(row0 + 1, rel_rows), :], turn, 1)
        win[b] = jnp.where(lane_row < turn, now, after)
        wait_for(v_hbm, vb, b, 4 + batch)
        scores = []
        for c in range(tiles):
            rel = jnp.concatenate([jnp.broadcast_to(win[b, c:c + 1, :], (heads, LANES)),
                                   jnp.broadcast_to(win[b, tiles + c:tiles + c + 1, :], (heads, LANES))], axis=0)
            s = (sc[b, :, c * LANES:(c + 1) * LANES] + rel) * scale
            scores.append(jnp.where(slot < n - c * per_row, s, MASKED))
        top = functools.reduce(jnp.maximum, scores)
        top = jnp.max(top, axis=1, keepdims=True)
        top = jnp.maximum(jnp.maximum(top[:heads], top[heads:]), FLOOR)
        top2 = jnp.concatenate([top, top], axis=0)
        weights = [jnp.exp(s - top2) for s in scores]
        total = jnp.sum(functools.reduce(jnp.add, weights), axis=1, keepdims=True)
        total = total[:heads] + total[heads:]
        acc = jnp.zeros((2 * heads, 2 * head_dim), F32)
        for c in range(half // 256):
            values = jnp.concatenate([vb[b, c * 256:(c + 1) * 256, :], vb[b, half + c * 256:half + (c + 1) * 256, :]], axis=1)
            p = jnp.concatenate([weights[2 * c], weights[2 * c + 1]], axis=1).astype(BF16)
            acc = acc + jnp.dot(p, values, preferred_element_type=F32)
        ctx = acc[:heads, :head_dim] + acc[heads:, head_dim:]
        csend[:, 0, pl.ds(b, 1), :] = ctx.reshape(heads, 1, head_dim)
        stats = jnp.where(first_stat, top, total)
        csend[:, 1, pl.ds(b, 1), :] = stats.reshape(heads, 1, LANES)
        return carry

    lax.fori_loop(0, batch, attend, 0)

    scatter(3, csend, crecv)
    crecv[me] = csend[me]

    arrived(1, kvrecv)
    k_new, v_new = kvrecv[0, 0], kvrecv[0, 1]
    for p in range(1, n_sp):
        k_new, v_new = k_new + kvrecv[p, 0], v_new + kvrecv[p, 1]
    k_new = k_new.astype(BF16).astype(F32)
    v_new = v_new.astype(BF16).astype(F32)
    q_cont = (qall[me] + jnp.sum(jnp.where(lax.broadcasted_iota(jnp.int32, (heads, head_dim), 0) == me, u_wide, 0.0), axis=0, keepdims=True))
    q_cont = q_cont.astype(BF16).astype(F32)
    last_row = (n_sp - 1 - me) * rel_rows + rel_rows - 1
    zero_dist = grid_rel[:, pl.ds(last_row, 1), :].reshape(batch, LANES)
    lane_b = lax.broadcasted_iota(jnp.int32, (batch, LANES), 1)
    rel0 = jnp.sum(jnp.where(lane_b == LANES - heads + me, zero_dist, 0.0), axis=1, keepdims=True)
    s_new = (jnp.sum(q_cont * k_new, axis=1, keepdims=True) + rel0) * scale

    arrived(3, crecv)
    tops = [crecv[p, 1][:, :1] for p in range(n_sp)]
    sums = [crecv[p, 1][:, LANES - 1:] for p in range(n_sp)]
    best = functools.reduce(jnp.maximum, tops, s_new)
    e_new = jnp.exp(s_new - best)
    denom = e_new
    numer = e_new.astype(BF16).astype(F32) * v_new
    for p in range(n_sp):
        factor = jnp.exp(tops[p] - best)
        denom = denom + factor * sums[p]
        numer = numer + factor * crecv[p, 0]
    call[me] = (numer / denom).astype(BF16).astype(F32)
    gather(4, call)
    arrived(4, call)

    ctx_all = jnp.concatenate([call[h].astype(BF16) for h in range(heads)], axis=1)
    wo_copy.wait()
    aosend[...] = jnp.dot(ctx_all, wob[...], preferred_element_type=F32)
    attn = tp_sum(0, aosend, aorecv)
    x1 = (hid[:, o_cols].astype(F32) + attn).astype(BF16).astype(F32)
    x1all[me] = x1
    gather(5, x1all)
    arrived(5, x1all)

    x1_parts = [x1all[p] for p in range(n_sp)]
    mean_sq = functools.reduce(jnp.add, [jnp.sum(t * t, axis=-1, keepdims=True) for t in x1_parts]) / (co * n_sp)
    inv = lax.rsqrt(mean_sq + EPS)
    normed = jnp.concatenate([(t * inv * gm[:, p * co:(p + 1) * co].astype(F32)).astype(BF16) for p, t in enumerate(x1_parts)], axis=1)
    wu_copy.wait()
    up = jnp.dot(normed, wub[...], preferred_element_type=F32)
    aall[me] = jax.nn.gelu(up, approximate=True).astype(BF16).astype(F32)
    gather(6, aall)
    arrived(6, aall)
    act = jnp.concatenate([aall[p].astype(BF16) for p in range(n_sp)], axis=1)
    wd_copy.wait()
    dnsend[...] = jnp.dot(act, wdb[...], preferred_element_type=F32)
    down = tp_sum(1, dnsend, dnrecv)
    oall[me] = (x1all[me] + down).astype(BF16).astype(F32)
    gather(7, oall)
    arrived(7, oall)
    for p in range(n_sp):
        out_ref[:, p * co:(p + 1) * co] = oall[p].astype(BF16)

    for copy in sends:
        copy.wait_send()
    for off in range(1, n_sp):
        peer = sp_peer(off)

        @pl.when(peer + me <= n_sp - 1)
        def _():
            remote(relsend, rel_slot(me, peer), rel_ssem.at[peer], rel_rsem.at[me], {'sp': peer}).wait_send()


def solution(mesh):
    n_sp, n_tp = mesh.shape['sp'], mesh.shape['tp']
    spec_rows = P('dp', None)
    spec_cache = P('dp', 'sp', 'tp', None)
    in_specs = (spec_rows, spec_cache, spec_cache, P('dp'), P('sp', 'tp', None), P('tp', None), P('tp', None), P(None), P(None, 'tp', None), P(None, 'tp', None), P(None, 'tp', None), P('tp', None, None), P(None), P(None, 'tp'), P('tp', None))
    out_specs = spec_rows

    def layer_step(hidden, k_cache, v_cache, lengths, rel_table, u_bias, w_bias, g_attn, w_query, w_key, w_value, w_out, g_mlp, w_up, w_down):
        batch, seq_blk, heads, head_dim = k_cache.shape
        width = hidden.shape[1]
        ff = w_up.shape[1]
        rows = seq_blk * heads
        kk = width // n_sp
        co = width // n_sp
        cf = ff // n_sp
        rel_rows = rows // LANES
        vmem = functools.partial(pl.BlockSpec, memory_space=pltpu.VMEM)
        hbm = functools.partial(pl.BlockSpec, memory_space=pl.ANY)
        dma = pltpu.SemaphoreType.DMA
        phases = 8
        return pl.pallas_call(
            functools.partial(layer_kernel, n_sp, n_tp),
            out_shape=jax.ShapeDtypeStruct((batch, width), BF16),
            in_specs=[pl.BlockSpec(memory_space=pltpu.SMEM)] + [vmem()] * 5 + [hbm()] * 9,
            out_specs=vmem(),
            scratch_shapes=[
                pltpu.VMEM((3, kk * heads, head_dim), BF16),
                pltpu.VMEM((seq_blk, heads, head_dim), BF16),
                pltpu.VMEM((rows, head_dim), BF16),
                pltpu.VMEM((batch, rows, head_dim), BF16),
                pltpu.VMEM((batch, rows, head_dim), BF16),
                pltpu.VMEM((heads * head_dim, co), BF16),
                pltpu.VMEM((width, cf), BF16),
                pltpu.VMEM((ff, co), BF16),
                pltpu.VMEM((n_sp, batch, head_dim), F32),
                pltpu.VMEM((n_sp, batch, head_dim), F32),
                pltpu.VMEM((n_sp, 2, batch, head_dim), F32),
                pltpu.VMEM((n_sp, 2, batch, head_dim), F32),
                pltpu.VMEM((n_sp, batch, head_dim), F32),
                pltpu.VMEM((batch, heads, head_dim), F32),
                pltpu.VMEM((batch, rel_rows, LANES), F32),
                pltpu.VMEM((batch, n_sp * rel_rows + 8, LANES), F32),
                pltpu.VMEM((batch, rel_rows, LANES), F32),
                pltpu.VMEM((batch, 2 * heads, rows // 2), F32),
                pltpu.VMEM((n_sp, 2, batch, head_dim), F32),
                pltpu.VMEM((n_sp, 2, batch, head_dim), F32),
                pltpu.VMEM((n_sp, batch, head_dim), F32),
                pltpu.VMEM((batch, co), F32),
                pltpu.VMEM((n_tp, batch, co), F32),
                pltpu.VMEM((n_sp, batch, co), F32),
                pltpu.VMEM((n_sp, batch, cf), F32),
                pltpu.VMEM((batch, co), F32),
                pltpu.VMEM((n_tp, batch, co), F32),
                pltpu.VMEM((n_sp, batch, co), F32),
                dma((7 + 2 * batch,)),
                dma((phases, n_sp)),
                dma((phases, n_sp)),
                dma((n_sp,)),
                dma((n_sp,)),
                dma((2, n_tp)),
                dma((2, n_tp)),
            ],
            compiler_params=pltpu.CompilerParams(collective_id=0, has_side_effects=True, vmem_limit_bytes=67043328),
            name='decode_layer',
        )(lengths, hidden, u_bias, w_bias, g_attn.reshape(1, width), g_mlp.reshape(1, width), rel_table,
          k_cache.reshape(batch, rows, head_dim), v_cache.reshape(batch, rows, head_dim),
          w_query.reshape(width * heads, head_dim), w_key.reshape(width * heads, head_dim), w_value.reshape(width * heads, head_dim),
          w_out.reshape(heads * head_dim, width), w_up, w_down)

    return jax.shard_map(layer_step, mesh=mesh, in_specs=in_specs, out_specs=out_specs, check_vma=False)
```

```python
import functools

import jax
import jax.numpy as jnp
from jax import lax
from jax.experimental import pallas as pl
from jax.experimental.pallas import tpu as pltpu
from jax.sharding import PartitionSpec as P

EPS = 1e-6
MASKED = -1e30
CORES = 2
CHUNKS = 4
FLOOR = -5e29
LANES = 128
F32 = jnp.float32
BF16 = jnp.bfloat16
NT = (((1,), (1,)), ((), ()))


def layer_kernel(n_sp, n_tp,
                 lens, hid, u_ref, w_ref, ga, gm, rel_hbm, k_hbm, v_hbm, wq_hbm, wk_hbm, wv_hbm, wo_hbm, wu_hbm, wd_hbm,
                 out_ref,
                 wqb, wkvb, normed, relb, rrev, kb, vb, wob, wub, wdb,
                 kvsend, kvrecv, qall, qcb, relsend, grid_rel0, grid_rel1, grid_rel2, grid_rel3, win, sc, csend, crecv, call, aosend, aorecv,
                 x1all, aall, dnsend, dnrecv, oall,
                 hsem, ssem, rsem, rel_ssem, rel_rsem, fwd_ssem, fwd_rsem, relay_ssem, sib_ssem, sib_rsem, tp_ssem, tp_rsem):
    me = lax.axis_index('sp')
    my_tp = lax.axis_index('tp')
    batch = hid.shape[0]
    heads = u_ref.shape[0]
    head_dim = u_ref.shape[1]
    rows = kb.shape[1]
    seq_blk = rows // heads
    kk = wkvb.shape[1] // heads
    pieces = 8
    chunks = CHUNKS
    chunk = batch // chunks
    chips = n_sp // CORES
    chip, core = me // CORES, me % CORES
    sibling = chip * CORES + 1 - core
    co = wob.shape[1]
    per_row = LANES // heads
    rel_rows = seq_blk // per_row
    smax = seq_blk * n_sp
    half = rows // 2
    scale = head_dim ** -0.5

    grid_rel = (grid_rel0, grid_rel1, grid_rel2, grid_rel3)
    marks = []

    def mark(name):
        if marks:
            marks.pop().__exit__(None, None, None)
        if name:
            scope = jax.named_scope(name)
            scope.__enter__()
            marks.append(scope)

    copies = []

    def fetch(src, dst):
        copy = pltpu.make_async_copy(src, dst, hsem.at[len(copies)])
        copies.append(copy)
        copy.start()
        return copy

    piece = wqb.shape[0] // pieces
    q_copies = [fetch(wq_hbm.at[i * piece:(i + 1) * piece], wqb.at[i * piece:(i + 1) * piece]) for i in range(pieces)]
    rel_copy = fetch(rel_hbm, relb)
    w_rows = pl.ds(pl.multiple_of(me * kk * heads, kk * heads), kk * heads)
    w_copies = [fetch(src.at[w_rows], wkvb.at[i]) for i, src in enumerate((wk_hbm, wv_hbm))]
    first_k = len(copies)
    for b in range(batch):
        fetch(k_hbm.at[b], kb.at[b])
    first_v = len(copies)
    for b in range(batch):
        fetch(v_hbm.at[b], vb.at[b])
    o_cols = pl.ds(pl.multiple_of(me * co, co), co)
    wo_copy = fetch(wo_hbm.at[:, o_cols], wob)
    f_cols = pl.ds(pl.multiple_of(me * wub.shape[1], wub.shape[1]), wub.shape[1])
    wu_copy = fetch(wu_hbm.at[:, f_cols], wub)
    wd_copy = fetch(wd_hbm.at[:, o_cols], wdb)

    def sp_peer(off):
        return lax.rem(me + off, n_sp)

    def tp_peer(off):
        return lax.rem(my_tp + off, n_tp)

    mark('zero')
    for part in grid_rel:
        part[...] = jnp.zeros_like(part)

    barrier = pltpu.get_barrier_semaphore()
    for off in range(1, n_sp):
        pl.semaphore_signal(barrier, inc=1, device_id={'sp': sp_peer(off)}, device_id_type=pl.DeviceIdType.MESH)
    for off in range(1, n_tp):
        pl.semaphore_signal(barrier, inc=1, device_id={'tp': tp_peer(off)}, device_id_type=pl.DeviceIdType.MESH)

    def remote(src, dst, send, recv, where):
        return pltpu.make_async_remote_copy(src_ref=src, dst_ref=dst, send_sem=send, recv_sem=recv, device_id=where,
                                            device_id_type=pl.DeviceIdType.MESH)

    sends = []

    def scatter(phase, src, dst):
        for off in range(1, n_sp):
            peer = sp_peer(off)
            copy = remote(src.at[peer], dst.at[me], ssem.at[phase, peer], rsem.at[phase, me], {'sp': peer})
            copy.start()
            sends.append(copy)

    def gather(phase, buf):
        for off in range(1, n_sp):
            peer = sp_peer(off)
            copy = remote(buf.at[me], buf.at[me], ssem.at[phase, peer], rsem.at[phase, me], {'sp': peer})
            copy.start()
            sends.append(copy)

    def arrived(phase, buf):
        for off in range(1, n_sp):
            peer = sp_peer(off)
            remote(buf.at[peer], buf.at[peer], ssem.at[phase, peer], rsem.at[phase, peer], {'sp': peer}).wait_recv()

    def tp_sum(phase, src, dst):
        dst[my_tp] = src[...]
        for off in range(1, n_tp):
            peer = tp_peer(off)
            copy = remote(src, dst.at[my_tp], tp_ssem.at[phase, peer], tp_rsem.at[phase, my_tp], {'tp': peer})
            copy.start()
            sends.append(copy)
        for off in range(1, n_tp):
            peer = tp_peer(off)
            remote(src, dst.at[peer], tp_ssem.at[phase, peer], tp_rsem.at[phase, peer], {'tp': peer}).wait_recv()
        total = dst[0]
        for t in range(1, n_tp):
            total = total + dst[t]
        return total

    mark('norm')
    wide = hid[...].astype(F32)
    inv = lax.rsqrt(jnp.mean(wide * wide, axis=-1, keepdims=True) + EPS)
    whole = (wide * inv * ga[...].reshape(1, wide.shape[1]).astype(F32)).astype(BF16)
    for c in range(wide.shape[1] // LANES):
        normed[c] = whole[:, c * LANES:(c + 1) * LANES]

    mark('qproj')
    span = LANES * heads
    spread = (lax.broadcasted_iota(jnp.int32, (LANES, span), 1) // heads
              == lax.broadcasted_iota(jnp.int32, (LANES, span), 0)).astype(F32).astype(BF16)
    lane_head = lax.broadcasted_iota(jnp.int32, (batch, LANES), 1) % heads
    head_mask = [jnp.concatenate([(lane_head == h).astype(F32).astype(BF16)] * heads, axis=1) for h in range(heads)]

    def by_head(c):
        spread_in = jnp.dot(normed[c], spread, preferred_element_type=F32).astype(BF16)
        return jnp.concatenate([spread_in * head_mask[h] for h in range(heads)], axis=0)

    def project(i, acc):
        pltpu.make_async_copy(wq_hbm.at[pl.ds(0, piece)], wqb.at[pl.ds(0, piece)], hsem.at[i]).wait()
        per = piece // span
        for j in range(per):
            at = pl.multiple_of((i * per + j) * span, span)
            acc = acc + jnp.dot(by_head(i * per + j), wqb[pl.ds(at, span), :], preferred_element_type=F32)
        return acc

    acc = lax.fori_loop(0, pieces, project, jnp.zeros((heads * batch, head_dim), F32))
    for h in range(heads):
        qall[h] = acc[h * batch:(h + 1) * batch].astype(BF16).astype(F32)

    mark('reverse')
    rel_copy.wait()
    group = 32

    def reverse(i, carry):
        tile = relb[pl.ds(pl.multiple_of(i * group, group), group)].astype(F32)
        flipped = jnp.concatenate([tile[group - 1 - j:group - j] for j in range(group)], axis=0)
        flipped = flipped.reshape(group * heads, head_dim).astype(BF16)
        at = pl.multiple_of((seq_blk // group - 1 - i) * group * heads, group * heads)
        rrev[pl.ds(at, group * heads), :] = flipped
        return carry

    lax.fori_loop(0, seq_blk // group, reverse, 0)

    mark('rel')
    u_wide, w_wide = u_ref[...].astype(F32), w_ref[...].astype(F32)
    q_pos = jnp.concatenate([(qall[h] + w_wide[h:h + 1]).astype(BF16) for h in range(heads)], axis=0)

    def relative(c, carry):
        tiles_now = 4
        wide_span = tiles_now * LANES
        table = rrev[pl.ds(pl.multiple_of(c * wide_span, wide_span), wide_span), :]
        scores = lax.dot_general(q_pos, table, NT, preferred_element_type=F32)
        for t in range(tiles_now):
            tile = scores[:, t * LANES:(t + 1) * LANES]
            row = tile[:batch]
            for h in range(1, heads):
                row = jnp.where(lane_head == h, tile[h * batch:(h + 1) * batch], row)
            relsend[:, pl.ds(tiles_now * c + t, 1), :] = row.reshape(batch, 1, LANES)
        return carry

    lax.fori_loop(0, rows // (4 * LANES), relative, 0)

    mark('barrier')
    half_rows = rel_rows // CORES

    def seqs(g):
        return pl.ds(g * chunk, chunk)

    def spot(src, to_chip, g, first, size):
        at = (n_sp - 1 - src - CORES * to_chip) * rel_rows + first
        return grid_rel[g].at[:, pl.ds(pl.multiple_of(at, half_rows), size), :]

    def needed(a, b):
        return a + b <= chips - 1

    def rel_out(g, act):
        for dx in range(1, chips):
            to_chip = lax.rem(chip + dx, chips)

            @pl.when(needed(to_chip, chip))
            def _():
                for part in range(CORES):
                    if 2 * dx == chips and part == 1:
                        continue
                    act(remote(relsend.at[seqs(g), part * half_rows:(part + 1) * half_rows, :],
                               spot(me, to_chip, g, part * half_rows, half_rows),
                               rel_ssem.at[dx, g, part], rel_rsem.at[me, g], {'sp': to_chip * CORES + part}))

        @pl.when(needed(chip, chip))
        def _():
            act(remote(relsend.at[seqs(g)], spot(me, chip, g, 0, rel_rows), sib_ssem.at[g], sib_rsem.at[g], {'sp': sibling}))

    def each_source(fn):
        for dx in range(1, chips):
            from_chip = lax.rem(chip + dx, chips)

            @pl.when(needed(from_chip, chip))
            def _():
                for c in range(CORES):
                    fn(dx, from_chip, c)

    def pass_on(g, dx, from_chip, c, act):
        src = from_chip * CORES + c
        mine = spot(src, chip, g, core * half_rows, half_rows)
        act(remote(mine, mine, fwd_ssem.at[dx, c, g], fwd_rsem.at[src, g], {'sp': sibling}))
        if dx == 1:
            to_chip = lax.rem(chip + chips - 1, chips)

            @pl.when(jnp.logical_and(core == 1, needed(to_chip, from_chip)))
            def _():
                act(remote(mine, spot(src, to_chip, g, half_rows, half_rows), relay_ssem.at[c, g], rel_rsem.at[src, g],
                           {'sp': to_chip * CORES + 1}))

    def rel_in(g):
        def fn(dx, from_chip, c):
            src = from_chip * CORES + c
            mine = spot(src, chip, g, core * half_rows, half_rows)
            remote(mine, mine, fwd_ssem.at[dx, c, g], rel_rsem.at[src, g], {'sp': sibling}).wait_recv()
            pass_on(g, dx, from_chip, c, lambda copy: copy.start())

        each_source(fn)

    def rel_done(g):
        def fn(dx, from_chip, c):
            src = from_chip * CORES + c
            other = spot(src, chip, g, (1 - core) * half_rows, half_rows)
            remote(other, other, fwd_ssem.at[dx, c, g], fwd_rsem.at[src, g], {'sp': sibling}).wait_recv()

        each_source(fn)

        @pl.when(needed(chip, chip))
        def _():
            block = spot(sibling, chip, g, 0, rel_rows)
            remote(block, block, sib_ssem.at[g], sib_rsem.at[g], {'sp': sibling}).wait_recv()

    pl.semaphore_wait(barrier, n_sp + n_tp - 2)
    mark('relout')
    for g in range(chunks):
        rel_out(g, lambda copy: copy.start())

    @pl.when(needed(chip, chip))
    def _():
        at = pl.multiple_of((n_sp - 1 - me - CORES * chip) * rel_rows, rel_rows)
        for g in range(chunks):
            grid_rel[g][:, pl.ds(at, rel_rows), :] = relsend[seqs(g)]

    mark('kv')
    for i in range(2):
        w_copies[i].wait()
    lhs_first = me * (kk // LANES)
    acc = [jnp.zeros((heads * batch, head_dim), F32)] * 2
    for c in range(kk // LANES):
        lhs = by_head(lhs_first + c)
        acc = [acc[i] + jnp.dot(lhs, wkvb[i, c * span:(c + 1) * span, :], preferred_element_type=F32) for i in range(2)]
    for i in range(2):
        for h in range(heads):
            kvsend[h, i] = acc[i][h * batch:(h + 1) * batch]
    scatter(1, kvsend, kvrecv)
    kvrecv[me] = kvsend[me]

    mark('content')
    for h in range(heads):
        qcb[:, h:h + 1, :] = (qall[h] + u_wide[h:h + 1]).reshape(batch, 1, head_dim)

    def wait_for(copy_src, copy_dst, b, first):
        pltpu.make_async_copy(copy_src.at[b], copy_dst.at[b], hsem.at[first + b]).wait()

    def content(b, carry):
        wait_for(k_hbm, kb, b, first_k)
        q = qcb[b]
        zero = jnp.zeros_like(q)
        two = jnp.concatenate([jnp.concatenate([q, zero], axis=1), jnp.concatenate([zero, q], axis=1)], axis=0).astype(BF16)
        for c in range(half // 256):
            keys = jnp.concatenate([kb[b, c * 256:(c + 1) * 256, :], kb[b, half + c * 256:half + (c + 1) * 256, :]], axis=1)
            sc[b, :, c * 256:(c + 1) * 256] = lax.dot_general(two, keys, NT, preferred_element_type=F32)
        return carry

    r_iota = lax.broadcasted_iota(jnp.int32, (2 * heads, LANES), 0)
    l_iota = lax.broadcasted_iota(jnp.int32, (2 * heads, LANES), 1)
    slot = me * seq_blk + (r_iota // heads) * (seq_blk // 2) + l_iota // heads
    slot = jnp.where(r_iota % heads == l_iota % heads, slot, jnp.int32(2 ** 30))
    lane_row = lax.broadcasted_iota(jnp.int32, (rel_rows, LANES), 1)
    first_stat = lax.broadcasted_iota(jnp.int32, (heads, LANES), 1) < LANES // 2
    tiles = half // LANES

    def attend(g, j, carry):
        b = g * chunk + j
        n = lens[b]
        start = smax - 1 - n
        row0 = jnp.minimum(start // per_row + core * rel_rows, n_sp * rel_rows - 1)
        turn = LANES - heads * (start % per_row)
        now = pltpu.roll(grid_rel[g][j, pl.ds(row0, rel_rows), :], turn, 1)
        after = pltpu.roll(grid_rel[g][j, pl.ds(row0 + 1, rel_rows), :], turn, 1)
        win[b] = jnp.where(lane_row < turn, now, after)
        wait_for(v_hbm, vb, b, first_v)
        scores = []
        for c in range(tiles):
            rel = jnp.concatenate([jnp.broadcast_to(win[b, c:c + 1, :], (heads, LANES)),
                                   jnp.broadcast_to(win[b, tiles + c:tiles + c + 1, :], (heads, LANES))], axis=0)
            s = (sc[b, :, c * LANES:(c + 1) * LANES] + rel) * scale
            scores.append(jnp.where(slot < n - c * per_row, s, MASKED))
        top = functools.reduce(jnp.maximum, scores)
        top = jnp.max(top, axis=1, keepdims=True)
        top = jnp.maximum(jnp.maximum(top[:heads], top[heads:]), FLOOR)
        top2 = jnp.concatenate([top, top], axis=0)
        weights = [jnp.exp(s - top2) for s in scores]
        total = jnp.sum(functools.reduce(jnp.add, weights), axis=1, keepdims=True)
        total = total[:heads] + total[heads:]
        acc = jnp.zeros((2 * heads, 2 * head_dim), F32)
        for c in range(half // 256):
            values = jnp.concatenate([vb[b, c * 256:(c + 1) * 256, :], vb[b, half + c * 256:half + (c + 1) * 256, :]], axis=1)
            p = jnp.concatenate([weights[2 * c], weights[2 * c + 1]], axis=1).astype(BF16)
            acc = acc + jnp.dot(p, values, preferred_element_type=F32)
        ctx = acc[:heads, :head_dim] + acc[heads:, head_dim:]
        csend[:, 0, pl.ds(b, 1), :] = ctx.reshape(heads, 1, head_dim)
        stats = jnp.where(first_stat, top, total)
        csend[:, 1, pl.ds(b, 1), :] = stats.reshape(heads, 1, LANES)
        return carry

    def content_of(g):
        lax.fori_loop(g * chunk, (g + 1) * chunk, content, 0)

    def attend_of(g):
        lax.fori_loop(0, chunk, functools.partial(attend, g), 0)

    mark('content01')
    content_of(0)
    content_of(1)
    mark('relin0')
    rel_in(0)
    mark('content2')
    content_of(2)
    mark('relin1')
    rel_in(1)
    mark('content3')
    content_of(3)
    for g in range(chunks):
        if g + 2 < chunks:
            mark(f'relin{g + 2}')
            rel_in(g + 2)
        mark(f'reldone{g}')
        rel_done(g)
        mark(f'attend{g}')
        attend_of(g)

    mark('ctxsend')
    scatter(3, csend, crecv)
    crecv[me] = csend[me]

    mark('newtok')
    arrived(1, kvrecv)
    k_new, v_new = kvrecv[0, 0], kvrecv[0, 1]
    for p in range(1, n_sp):
        k_new, v_new = k_new + kvrecv[p, 0], v_new + kvrecv[p, 1]
    k_new = k_new.astype(BF16).astype(F32)
    v_new = v_new.astype(BF16).astype(F32)
    q_cont = (qall[me] + jnp.sum(jnp.where(lax.broadcasted_iota(jnp.int32, (heads, head_dim), 0) == me, u_wide, 0.0), axis=0, keepdims=True))
    q_cont = q_cont.astype(BF16).astype(F32)
    last_row = (n_sp - 1 - CORES * chip) * rel_rows + rel_rows - 1
    zero_dist = jnp.concatenate([part[:, pl.ds(last_row, 1), :].reshape(chunk, LANES) for part in grid_rel], axis=0)
    lane_b = lax.broadcasted_iota(jnp.int32, (batch, LANES), 1)
    rel0 = jnp.sum(jnp.where(lane_b == LANES - heads + me, zero_dist, 0.0), axis=1, keepdims=True)
    s_new = (jnp.sum(q_cont * k_new, axis=1, keepdims=True) + rel0) * scale

    mark('ctxwait')
    arrived(3, crecv)
    mark('combine')
    tops = [crecv[p, 1][:, :1] for p in range(n_sp)]
    sums = [crecv[p, 1][:, LANES - 1:] for p in range(n_sp)]
    best = functools.reduce(jnp.maximum, tops, s_new)
    e_new = jnp.exp(s_new - best)
    denom = e_new
    numer = e_new.astype(BF16).astype(F32) * v_new
    for p in range(n_sp):
        factor = jnp.exp(tops[p] - best)
        denom = denom + factor * sums[p]
        numer = numer + factor * crecv[p, 0]
    call[me] = (numer / denom).astype(BF16).astype(F32)
    mark('agctx')
    gather(4, call)
    mark('agctxwait')
    arrived(4, call)

    mark('oproj')
    ctx_all = jnp.concatenate([call[h].astype(BF16) for h in range(heads)], axis=1)
    wo_copy.wait()
    aosend[...] = jnp.dot(ctx_all, wob[...], preferred_element_type=F32)
    mark('tpsum')
    attn = tp_sum(0, aosend, aorecv)
    mark('x1')
    x1 = (hid[:, o_cols].astype(F32) + attn).astype(BF16).astype(F32)
    x1all[me] = x1
    mark('agx1')
    gather(5, x1all)
    mark('agx1wait')
    arrived(5, x1all)

    mark('mlpnorm')
    x1_parts = [x1all[p] for p in range(n_sp)]
    mean_sq = functools.reduce(jnp.add, [jnp.sum(t * t, axis=-1, keepdims=True) for t in x1_parts]) / (co * n_sp)
    inv = lax.rsqrt(mean_sq + EPS)
    gain = gm[...].reshape(1, co * n_sp).astype(F32)
    normed_mid = jnp.concatenate([(t * inv * gain[:, p * co:(p + 1) * co]).astype(BF16) for p, t in enumerate(x1_parts)], axis=1)
    mark('up')
    wu_copy.wait()
    up = jnp.dot(normed_mid, wub[...], preferred_element_type=F32)
    aall[me] = jax.nn.gelu(up, approximate=True).astype(BF16).astype(F32)
    mark('aga')
    gather(6, aall)
    mark('agawait')
    arrived(6, aall)
    mark('down')
    act = jnp.concatenate([aall[p].astype(BF16) for p in range(n_sp)], axis=1)
    wd_copy.wait()
    dnsend[...] = jnp.dot(act, wdb[...], preferred_element_type=F32)
    mark('tpsum2')
    down = tp_sum(1, dnsend, dnrecv)
    oall[me] = (x1all[me] + down).astype(BF16).astype(F32)
    mark('ago')
    gather(7, oall)
    mark('agowait')
    arrived(7, oall)
    mark('outw')
    for p in range(n_sp):
        out_ref[:, p * co:(p + 1) * co] = oall[p].astype(BF16)

    mark('sendwait')
    for copy in sends:
        copy.wait_send()
    for g in range(chunks):
        rel_out(g, lambda copy: copy.wait_send())
        each_source(lambda dx, from_chip, c: pass_on(g, dx, from_chip, c, lambda copy: copy.wait_send()))
    mark('')


def solution(mesh):
    n_sp, n_tp = mesh.shape['sp'], mesh.shape['tp']
    spec_rows = P('dp', None)
    spec_cache = P('dp', 'sp', 'tp', None)
    in_specs = (spec_rows, spec_cache, spec_cache, P('dp'), P('sp', 'tp', None), P('tp', None), P('tp', None), P(None), P(None, 'tp', None), P(None, 'tp', None), P(None, 'tp', None), P('tp', None, None), P(None), P(None, 'tp'), P('tp', None))
    out_specs = spec_rows

    def layer_step(hidden, k_cache, v_cache, lengths, rel_table, u_bias, w_bias, g_attn, w_query, w_key, w_value, w_out, g_mlp, w_up, w_down):
        batch, seq_blk, heads, head_dim = k_cache.shape
        width = hidden.shape[1]
        ff = w_up.shape[1]
        rows = seq_blk * heads
        kk = width // n_sp
        co = width // n_sp
        cf = ff // n_sp
        rel_rows = rows // LANES
        vmem = functools.partial(pl.BlockSpec, memory_space=pltpu.VMEM)
        hbm = functools.partial(pl.BlockSpec, memory_space=pl.ANY)
        dma = pltpu.SemaphoreType.DMA
        phases = 8
        return pl.pallas_call(
            functools.partial(layer_kernel, n_sp, n_tp),
            out_shape=jax.ShapeDtypeStruct((batch, width), BF16),
            in_specs=[pl.BlockSpec(memory_space=pltpu.SMEM)] + [vmem()] * 5 + [hbm()] * 9,
            out_specs=vmem(),
            scratch_shapes=[
                pltpu.VMEM((width * heads, head_dim), BF16),
                pltpu.VMEM((2, kk * heads, head_dim), BF16),
                pltpu.VMEM((width // LANES, batch, LANES), BF16),
                pltpu.VMEM((seq_blk, heads, head_dim), BF16),
                pltpu.VMEM((rows, head_dim), BF16),
                pltpu.VMEM((batch, rows, head_dim), BF16),
                pltpu.VMEM((batch, rows, head_dim), BF16),
                pltpu.VMEM((heads * head_dim, co), BF16),
                pltpu.VMEM((width, cf), BF16),
                pltpu.VMEM((ff, co), BF16),
                pltpu.VMEM((n_sp, 2, batch, head_dim), F32),
                pltpu.VMEM((n_sp, 2, batch, head_dim), F32),
                pltpu.VMEM((n_sp, batch, head_dim), F32),
                pltpu.VMEM((batch, heads, head_dim), F32),
                pltpu.VMEM((batch, rel_rows, LANES), F32),
                *[pltpu.VMEM((batch // CHUNKS, (n_sp + 1) * rel_rows + 8, LANES), F32)] * CHUNKS,
                pltpu.VMEM((batch, rel_rows, LANES), F32),
                pltpu.VMEM((batch, 2 * heads, rows // 2), F32),
                pltpu.VMEM((n_sp, 2, batch, head_dim), F32),
                pltpu.VMEM((n_sp, 2, batch, head_dim), F32),
                pltpu.VMEM((n_sp, batch, head_dim), F32),
                pltpu.VMEM((batch, co), F32),
                pltpu.VMEM((n_tp, batch, co), F32),
                pltpu.VMEM((n_sp, batch, co), F32),
                pltpu.VMEM((n_sp, batch, cf), F32),
                pltpu.VMEM((batch, co), F32),
                pltpu.VMEM((n_tp, batch, co), F32),
                pltpu.VMEM((n_sp, batch, co), F32),
                dma((14 + 2 * batch,)),
                dma((phases, n_sp)),
                dma((phases, n_sp)),
                dma((n_sp // CORES, 4, CORES)),
                dma((n_sp, 4)),
                dma((n_sp // CORES, CORES, 4)),
                dma((n_sp, 4)),
                dma((CORES, 4)),
                dma((4,)),
                dma((4,)),
                dma((2, n_tp)),
                dma((2, n_tp)),
            ],
            compiler_params=pltpu.CompilerParams(collective_id=0, has_side_effects=True, vmem_limit_bytes=67043328),
            name='decode_layer',
        )(lengths, hidden, u_bias, w_bias, g_attn, g_mlp, rel_table,
          k_cache.reshape(batch, rows, head_dim), v_cache.reshape(batch, rows, head_dim),
          w_query.reshape(width * heads, head_dim), w_key.reshape(width * heads, head_dim), w_value.reshape(width * heads, head_dim),
          w_out.reshape(heads * head_dim, width), w_up, w_down)

    return jax.shard_map(layer_step, mesh=mesh, in_specs=in_specs, out_specs=out_specs, check_vma=False)
```

```python
import functools

import jax
import jax.numpy as jnp
from jax import lax
from jax.experimental import pallas as pl
from jax.experimental.pallas import tpu as pltpu
from jax.sharding import PartitionSpec as P

EPS = 1e-6
MASKED = -1e30
CORES = 2
CHUNKS = 4
UP_PARTS = 8
OUT_PARTS = 2
FLOOR = -5e29
LANES = 128
F32 = jnp.float32
BF16 = jnp.bfloat16
NT = (((1,), (1,)), ((), ()))


def layer_kernel(n_sp, n_tp,
                 lens_in, hid_in, u_in, w_in, ga_in, gm_in, rel_hbm, k_hbm, v_hbm, wq_hbm, wk_hbm, wv_hbm, wo_hbm, wu_hbm, wd_hbm,
                 out_ref,
                 lens, hid, u_ref, w_ref, ga, gm,
                 wqb, wkvb, normed, spread_x, relb, rrev, kb, vb, wob, wdb,
                 kvsend, kvrecv, qall, qcb, relsend, grid_rel0, grid_rel1, grid_rel2, grid_rel3, win, sc, csend, crecv, call, aosend, aorecv,
                 x1all, aall, dnsend, dnrecv, oall,
                 hsem, ssem, rsem, rel_ssem, rel_rsem, fwd_ssem, fwd_rsem, relay_ssem, sib_ssem, sib_rsem, ctx_ssem, ctx_rsem, a_ssem, a_rsem, tp_ssem, tp_rsem):
    me = lax.axis_index('sp')
    my_tp = lax.axis_index('tp')
    batch = hid.shape[0]
    heads = u_ref.shape[0]
    head_dim = u_ref.shape[1]
    rows = kb.shape[1]
    seq_blk = rows // heads
    kk = wkvb.shape[1] // heads
    pieces = 8
    chunks = CHUNKS
    chunk = batch // chunks
    chips = n_sp // CORES
    chip, core = me // CORES, me % CORES
    sibling = chip * CORES + 1 - core
    co = wob.shape[1]
    per_row = LANES // heads
    rel_rows = seq_blk // per_row
    smax = seq_blk * n_sp
    half = rows // 2
    half_ff = wu_hbm.shape[1] // CORES
    scale = head_dim ** -0.5

    grid_rel = (grid_rel0, grid_rel1, grid_rel2, grid_rel3)
    copies = []

    def fetch(src, dst, sem=None):
        copy = pltpu.make_async_copy(src, dst, hsem.at[len(copies) if sem is None else sem])
        if sem is None:
            copies.append(copy)
        copy.start()
        return copy

    small = [fetch(hid_in, hid), fetch(ga_in, ga), fetch(u_in, u_ref), fetch(w_in, w_ref), fetch(gm_in, gm), fetch(lens_in, lens)]
    rel_copy = fetch(rel_hbm, relb)
    first_q = len(copies)
    piece = wqb.shape[0] // pieces
    q_copies = [fetch(wq_hbm.at[i * piece:(i + 1) * piece], wqb.at[i * piece:(i + 1) * piece]) for i in range(pieces)]
    w_rows = pl.ds(pl.multiple_of(me * kk * heads, kk * heads), kk * heads)
    w_copies = [fetch(src.at[w_rows], wkvb.at[i]) for i, src in enumerate((wk_hbm, wv_hbm))]
    k_copies = [fetch(k_hbm.at[g * chunk:(g + 1) * chunk], kb.at[g * chunk:(g + 1) * chunk]) for g in range(chunks)]
    v_copies = [fetch(v_hbm.at[g * chunk:(g + 1) * chunk], vb.at[g * chunk:(g + 1) * chunk]) for g in range(chunks)]
    o_cols = pl.ds(pl.multiple_of(me * co, co), co)
    wo_copy = fetch(wo_hbm.at[:, o_cols], wob)
    wd_copy = fetch(wd_hbm.at[:, o_cols], wdb)

    peers = [(lax.rem(chip + dx, chips) * CORES + (core if e == 0 else 1 - core))
             for dx in sorted(range(chips), key=lambda d: -min(d, chips - d)) for e in range(CORES) if (dx, e) != (0, 0)]

    def tp_peer(off):
        return lax.rem(my_tp + off, n_tp)

    for part in grid_rel:
        part[...] = jnp.zeros_like(part)

    barrier = pltpu.get_barrier_semaphore()
    for peer in peers:
        pl.semaphore_signal(barrier, inc=1, device_id={'sp': peer}, device_id_type=pl.DeviceIdType.MESH)
    for off in range(1, n_tp):
        pl.semaphore_signal(barrier, inc=1, device_id={'tp': tp_peer(off)}, device_id_type=pl.DeviceIdType.MESH)

    def remote(src, dst, send, recv, where):
        return pltpu.make_async_remote_copy(src_ref=src, dst_ref=dst, send_sem=send, recv_sem=recv, device_id=where,
                                            device_id_type=pl.DeviceIdType.MESH)

    sends = []

    def later(src, sem):
        sends.append(lambda: remote(src, src, sem, sem, {'sp': sibling}).wait_send())

    def take(dst, sem):
        remote(dst, dst, sem, sem, {'sp': sibling}).wait_recv()

    others = slice(0, n_sp - 1)

    def scatter(phase, src, dst):
        for peer in peers:
            remote(src.at[peer], dst.at[me], ssem.at[phase], rsem.at[phase], {'sp': peer}).start()
        later(src.at[others], ssem.at[phase])

    def gather(phase, buf, part=None):
        block = buf.at[me] if part is None else buf.at[me, part]
        for peer in peers:
            remote(block, block, ssem.at[phase], rsem.at[phase], {'sp': peer}).start()
        if part is None or part == buf.shape[1] - 1:
            later(buf.at[others], ssem.at[phase])

    def arrived(phase, buf):
        take(buf.at[others], rsem.at[phase])

    def tp_send(phase, part, src, dst):
        dst[part, my_tp] = src[part]
        for off in sorted(range(1, n_tp), key=lambda d: -min(d, n_tp - d)):
            remote(src.at[part], dst.at[part, my_tp], tp_ssem.at[phase, part], tp_rsem.at[phase, part], {'tp': tp_peer(off)}).start()
        later(dst.at[part, 0:n_tp - 1], tp_ssem.at[phase, part])

    def tp_total(phase, part, dst):
        take(dst.at[part, 0:n_tp - 1], tp_rsem.at[phase, part])
        total = dst[part, 0]
        for t in range(1, n_tp):
            total = total + dst[part, t]
        return total

    for copy in small:
        copy.wait()
    wide = hid[...].astype(F32)
    inv = lax.rsqrt(jnp.mean(wide * wide, axis=-1, keepdims=True) + EPS)
    whole = (wide * inv * ga[...].reshape(1, wide.shape[1]).astype(F32)).astype(BF16)
    n_in = wide.shape[1] // LANES
    for c in range(n_in):
        normed[c * batch:(c + 1) * batch] = whole[:, c * LANES:(c + 1) * LANES]
    span = LANES * heads
    spread = (lax.broadcasted_iota(jnp.int32, (LANES, span), 1) // heads
              == lax.broadcasted_iota(jnp.int32, (LANES, span), 0)).astype(F32).astype(BF16)
    lane_head = lax.broadcasted_iota(jnp.int32, (batch, LANES), 1) % heads
    head_mask = [jnp.concatenate([(lane_head == h).astype(F32).astype(BF16)] * heads, axis=1) for h in range(heads)]

    spread_x[...] = jnp.dot(normed[...], spread, preferred_element_type=F32).astype(BF16)

    def by_head(c):
        spread_in = spread_x[pl.ds(pl.multiple_of(c * batch, batch), batch), :]
        return jnp.concatenate([spread_in * head_mask[h] for h in range(heads)], axis=0)

    rel_copy.wait()
    group = 32

    def reverse(i, carry):
        tile = relb[pl.ds(pl.multiple_of(i * group, group), group)].astype(F32)
        flipped = jnp.concatenate([tile[group - 1 - j:group - j] for j in range(group)], axis=0)
        flipped = flipped.reshape(group * heads, head_dim).astype(BF16)
        at = pl.multiple_of((seq_blk // group - 1 - i) * group * heads, group * heads)
        rrev[pl.ds(at, group * heads), :] = flipped
        return carry

    lax.fori_loop(0, seq_blk // group, reverse, 0)

    def project(i, acc):
        pltpu.make_async_copy(wq_hbm.at[pl.ds(0, piece)], wqb.at[pl.ds(0, piece)], hsem.at[first_q + i]).wait()
        per = piece // span
        for j in range(per):
            at = pl.multiple_of((i * per + j) * span, span)
            acc = acc + jnp.dot(by_head(i * per + j), wqb[pl.ds(at, span), :], preferred_element_type=F32)
        return acc

    acc = lax.fori_loop(0, pieces, project, jnp.zeros((heads * batch, head_dim), F32))
    for h in range(heads):
        qall[h] = acc[h * batch:(h + 1) * batch].astype(BF16).astype(F32)

    u_wide, w_wide = u_ref[...].astype(F32), w_ref[...].astype(F32)
    q_pos = jnp.concatenate([(qall[h] + w_wide[h:h + 1]).astype(BF16) for h in range(heads)], axis=0)

    def relative(c, carry):
        tiles_now = 4
        wide_span = tiles_now * LANES
        table = rrev[c * wide_span:(c + 1) * wide_span, :]
        scores = lax.dot_general(q_pos, table, NT, preferred_element_type=F32)
        for t in range(tiles_now):
            tile = scores[:, t * LANES:(t + 1) * LANES]
            row = tile[:batch]
            for h in range(1, heads):
                row = jnp.where(lane_head == h, tile[h * batch:(h + 1) * batch], row)
            at = tiles_now * c + t
            relsend[:, at:at + 1, :] = row.reshape(batch, 1, LANES)
        return carry

    for c in range(rows // (4 * LANES)):
        relative(c, 0)

    half_rows = rel_rows // CORES

    def seqs(g):
        return pl.ds(g * chunk, chunk)

    def spot(src, to_chip, g, first, size):
        at = (n_sp - 1 - src - CORES * to_chip) * rel_rows + first
        return grid_rel[g].at[:, pl.ds(pl.multiple_of(at, half_rows), size), :]

    def needed(a, b):
        return a + b <= chips - 1

    def rel_out(g, act):
        for dx in range(1, chips):
            to_chip = lax.rem(chip + dx, chips)

            @pl.when(needed(to_chip, chip))
            def _():
                for part in range(CORES):
                    if 2 * dx == chips and part == 1:
                        continue
                    act(remote(relsend.at[seqs(g), part * half_rows:(part + 1) * half_rows, :],
                               spot(me, to_chip, g, part * half_rows, half_rows),
                               rel_ssem.at[dx], rel_rsem.at[chip, g], {'sp': to_chip * CORES + part}))

        @pl.when(needed(chip, chip))
        def _():
            act(remote(relsend.at[seqs(g)], spot(me, chip, g, 0, rel_rows), sib_ssem.at[0], sib_rsem.at[g], {'sp': sibling}))

    def each_source(fn):
        for dx in range(1, chips):
            from_chip = lax.rem(chip + dx, chips)

            @pl.when(needed(from_chip, chip))
            def _():
                fn(dx, from_chip)

    def pass_on(g, dx, from_chip, c, act):
        src = from_chip * CORES + c
        mine = spot(src, chip, g, core * half_rows, half_rows)
        act(remote(mine, mine, fwd_ssem.at[dx], fwd_rsem.at[from_chip, g], {'sp': sibling}))
        if dx == 1:
            to_chip = lax.rem(chip + chips - 1, chips)

            @pl.when(jnp.logical_and(core == 1, needed(to_chip, from_chip)))
            def _():
                act(remote(mine, spot(src, to_chip, g, half_rows, half_rows), relay_ssem.at[0], rel_rsem.at[from_chip, g],
                           {'sp': to_chip * CORES + 1}))

    both = relsend.at[0:chunk]

    def rel_in(g):
        def fn(dx, from_chip):
            take(both, rel_rsem.at[from_chip, g])
            for c in range(CORES):
                pass_on(g, dx, from_chip, c, lambda copy: copy.start())

        each_source(fn)

    def rel_done(g):
        each_source(lambda dx, from_chip: take(both, fwd_rsem.at[from_chip, g]))

        @pl.when(needed(chip, chip))
        def _():
            take(both, sib_rsem.at[g])

    def rel_sent():
        for dx in range(1, chips):
            to_chip = lax.rem(chip + dx, chips)
            sent = relsend.at[:, 0:half_rows] if 2 * dx == chips else relsend

            @pl.when(needed(to_chip, chip))
            def _():
                remote(sent, sent, rel_ssem.at[dx], rel_ssem.at[dx], {'sp': sibling}).wait_send()
                remote(relsend, relsend, fwd_ssem.at[dx], fwd_ssem.at[dx], {'sp': sibling}).wait_send()

        @pl.when(needed(chip, chip))
        def _():
            remote(relsend, relsend, sib_ssem.at[0], sib_ssem.at[0], {'sp': sibling}).wait_send()

        to_chip, from_chip = lax.rem(chip + chips - 1, chips), lax.rem(chip + 1, chips)

        @pl.when(jnp.logical_and(jnp.logical_and(core == 1, needed(from_chip, chip)), needed(to_chip, from_chip)))
        def _():
            remote(relsend, relsend, relay_ssem.at[0], relay_ssem.at[0], {'sp': sibling}).wait_send()

    pl.semaphore_wait(barrier, n_sp + n_tp - 2)
    rel_out(0, lambda copy: copy.start())

    @pl.when(needed(chip, chip))
    def _():
        at = pl.multiple_of((n_sp - 1 - me - CORES * chip) * rel_rows, rel_rows)
        for g in range(chunks):
            grid_rel[g][:, pl.ds(at, rel_rows), :] = relsend[seqs(g)]

    for i in range(2):
        w_copies[i].wait()
    lhs_first = me * (kk // LANES)
    acc = [jnp.zeros((heads * batch, head_dim), F32)] * 2
    for c in range(kk // LANES):
        lhs = by_head(lhs_first + c)
        acc = [acc[i] + jnp.dot(lhs, wkvb[i, c * span:(c + 1) * span, :], preferred_element_type=F32) for i in range(2)]
    for i in range(2):
        for h in range(heads):
            kvsend[h, i] = acc[i][h * batch:(h + 1) * batch]
    scatter(0, kvsend, kvrecv)
    kvrecv[me] = kvsend[me]

    rel_out(1, lambda copy: copy.start())
    for h in range(heads):
        qcb[:, h:h + 1, :] = (qall[h] + u_wide[h:h + 1]).reshape(batch, 1, head_dim)

    def content_of(g):
        k_copies[g].wait()
        for j in range(chunk):
            b = g * chunk + j
            q = qcb[b]
            zero = jnp.zeros_like(q)
            two = jnp.concatenate([jnp.concatenate([q, zero], axis=1), jnp.concatenate([zero, q], axis=1)], axis=0).astype(BF16)
            for c in range(half // 256):
                keys = jnp.concatenate([kb[b, c * 256:(c + 1) * 256, :], kb[b, half + c * 256:half + (c + 1) * 256, :]], axis=1)
                sc[b, :, c * 256:(c + 1) * 256] = lax.dot_general(two, keys, NT, preferred_element_type=F32)

    r_iota = lax.broadcasted_iota(jnp.int32, (2 * heads, LANES), 0)
    l_iota = lax.broadcasted_iota(jnp.int32, (2 * heads, LANES), 1)
    slot = me * seq_blk + (r_iota // heads) * (seq_blk // 2) + l_iota // heads
    slot = jnp.where(r_iota % heads == l_iota % heads, slot, jnp.int32(2 ** 30))
    lane_row = lax.broadcasted_iota(jnp.int32, (rel_rows, LANES), 1)
    first_stat = lax.broadcasted_iota(jnp.int32, (heads, LANES), 1) < LANES // 2
    tiles = half // LANES

    def attend(g, j):
        b = g * chunk + j
        n = lens[b]
        start = smax - 1 - n
        row0 = jnp.minimum(start // per_row + core * rel_rows, n_sp * rel_rows - 1)
        turn = LANES - heads * (start % per_row)
        now = pltpu.roll(grid_rel[g][j, pl.ds(row0, rel_rows), :], turn, 1)
        after = pltpu.roll(grid_rel[g][j, pl.ds(row0 + 1, rel_rows), :], turn, 1)
        win[b] = jnp.where(lane_row < turn, now, after)
        scores = []
        for c in range(tiles):
            rel = jnp.concatenate([jnp.broadcast_to(win[b, c:c + 1, :], (heads, LANES)),
                                   jnp.broadcast_to(win[b, tiles + c:tiles + c + 1, :], (heads, LANES))], axis=0)
            s = (sc[b, :, c * LANES:(c + 1) * LANES] + rel) * scale
            scores.append(jnp.where(slot < n - c * per_row, s, MASKED))
        top = functools.reduce(jnp.maximum, scores)
        top = jnp.max(top, axis=1, keepdims=True)
        top = jnp.maximum(jnp.maximum(top[:heads], top[heads:]), FLOOR)
        top2 = jnp.concatenate([top, top], axis=0)
        weights = [jnp.exp(s - top2) for s in scores]
        total = jnp.sum(functools.reduce(jnp.add, weights), axis=1, keepdims=True)
        total = total[:heads] + total[heads:]
        acc = jnp.zeros((2 * heads, 2 * head_dim), F32)
        for c in range(half // 256):
            values = jnp.concatenate([vb[b, c * 256:(c + 1) * 256, :], vb[b, half + c * 256:half + (c + 1) * 256, :]], axis=1)
            p = jnp.concatenate([weights[2 * c], weights[2 * c + 1]], axis=1).astype(BF16)
            acc = acc + jnp.dot(p, values, preferred_element_type=F32)
        ctx = acc[:heads, :head_dim] + acc[heads:, head_dim:]
        csend[g, :, j:j + 1, :] = ctx.reshape(heads, 1, head_dim)
        stats = jnp.where(first_stat, top, total)
        csend[g, :, chunk + j:chunk + j + 1, :] = stats.reshape(heads, 1, LANES)

    def attend_of(g):
        for j in range(chunk):
            attend(g, j)
        for peer in peers:
            remote(csend.at[g, peer], crecv.at[g, me], ctx_ssem.at[0], ctx_rsem.at[0], {'sp': peer}).start()
        crecv[g, me] = csend[g, me]

    content_of(0)
    rel_out(2, lambda copy: copy.start())
    content_of(1)
    rel_out(3, lambda copy: copy.start())
    content_of(2)
    content_of(3)
    up_cols = half_ff // batch
    first_up = len(copies)
    up_groups = aall.shape[0] // CORES
    for t in range(batch):
        fetch(wu_hbm.at[:, pl.ds(pl.multiple_of(core * half_ff + t * up_cols, up_cols), up_cols)], kb.at[t],
              first_up + t // (batch // up_groups))
    for g in range(chunks):
        rel_in(g)
    for g in range(chunks):
        rel_done(g)
        v_copies[g].wait()
        attend_of(g)

    arrived(0, kvrecv)
    k_new, v_new = kvrecv[0, 0], kvrecv[0, 1]
    for p in range(1, n_sp):
        k_new, v_new = k_new + kvrecv[p, 0], v_new + kvrecv[p, 1]
    k_new = k_new.astype(BF16).astype(F32)
    v_new = v_new.astype(BF16).astype(F32)
    q_cont = (qall[me] + jnp.sum(jnp.where(lax.broadcasted_iota(jnp.int32, (heads, head_dim), 0) == me, u_wide, 0.0), axis=0, keepdims=True))
    q_cont = q_cont.astype(BF16).astype(F32)
    last_row = (n_sp - 1 - CORES * chip) * rel_rows + rel_rows - 1
    zero_dist = jnp.concatenate([part[:, pl.ds(last_row, 1), :].reshape(chunk, LANES) for part in grid_rel], axis=0)
    lane_b = lax.broadcasted_iota(jnp.int32, (batch, LANES), 1)
    rel0 = jnp.sum(jnp.where(lane_b == LANES - heads + me, zero_dist, 0.0), axis=1, keepdims=True)
    s_new = (jnp.sum(q_cont * k_new, axis=1, keepdims=True) + rel0) * scale

    later(csend.at[:, others], ctx_ssem.at[0])
    take(crecv.at[:, others], ctx_rsem.at[0])
    parts = [jnp.concatenate([crecv[g, p, :chunk] for g in range(chunks)], axis=0) for p in range(n_sp)]
    stats = [jnp.concatenate([crecv[g, p, chunk:] for g in range(chunks)], axis=0) for p in range(n_sp)]
    tops = [t[:, :1] for t in stats]
    sums = [t[:, LANES - 1:] for t in stats]
    best = functools.reduce(jnp.maximum, tops, s_new)
    e_new = jnp.exp(s_new - best)
    denom = e_new
    numer = e_new.astype(BF16).astype(F32) * v_new
    for p in range(n_sp):
        factor = jnp.exp(tops[p] - best)
        denom = denom + factor * sums[p]
        numer = numer + factor * parts[p]
    call[me] = (numer / denom).astype(BF16).astype(F32)
    gather(1, call)
    arrived(1, call)

    ctx_all = jnp.concatenate([call[h].astype(BF16) for h in range(heads)], axis=1)
    wo_copy.wait()
    parts_out, cp = aosend.shape[0], aosend.shape[2]
    attn_part = jnp.dot(ctx_all, wob[...], preferred_element_type=F32)
    for i in range(parts_out):
        aosend[i] = attn_part[:, i * cp:(i + 1) * cp]
        tp_send(0, i, aosend, aorecv)
    for i in range(parts_out):
        attn = tp_total(0, i, aorecv)
        x1_cols = pl.ds(pl.multiple_of(me * co + i * cp, cp), cp)
        x1all[me, i] = (hid[:, x1_cols].astype(F32) + attn).astype(BF16).astype(F32)
        gather(2, x1all, i)
    arrived(2, x1all)
    x1_parts = [x1all[p, i] for p in range(n_sp) for i in range(parts_out)]
    mean_sq = functools.reduce(jnp.add, [jnp.sum(t * t, axis=-1, keepdims=True) for t in x1_parts]) / (co * n_sp)
    inv = lax.rsqrt(mean_sq + EPS)
    gain = gm[...].reshape(1, co * n_sp).astype(F32)
    normed_mid = jnp.concatenate([(t * inv * gain[:, p * cp:(p + 1) * cp]).astype(BF16) for p, t in enumerate(x1_parts)], axis=1)
    per_part = aall.shape[2] // up_cols
    for i in range(aall.shape[0] // CORES):
        tiles_up = kb.at[i * per_part:(i + 1) * per_part]
        pltpu.make_async_copy(tiles_up, tiles_up, hsem.at[first_up + i]).wait()
        at = core * (aall.shape[0] // CORES) + i
        weights = jnp.concatenate([kb[t] for t in range(i * per_part, (i + 1) * per_part)], axis=1)
        up = jnp.dot(normed_mid, weights, preferred_element_type=F32)
        aall[at] = jax.nn.gelu(up, approximate=True).astype(BF16).astype(F32)
        remote(aall.at[at], aall.at[at], a_ssem.at[0], a_rsem.at[0], {'sp': sibling}).start()
    later(aall.at[0:up_groups], a_ssem.at[0])

    def down_of(which):
        act = jnp.concatenate([aall[which * up_groups + i].astype(BF16) for i in range(up_groups)], axis=1)
        units = pl.ds(pl.multiple_of(which * half_ff, half_ff), half_ff)
        return jnp.dot(act, wdb[units, :], preferred_element_type=F32)

    wd_copy.wait()
    down_part = down_of(core)
    take(aall.at[0:up_groups], a_rsem.at[0])
    down_part = down_part + down_of(1 - core)
    for i in range(parts_out):
        dnsend[i] = down_part[:, i * cp:(i + 1) * cp]
        tp_send(1, i, dnsend, dnrecv)
    for i in range(parts_out):
        down = tp_total(1, i, dnrecv)
        oall[me, i] = (x1all[me, i] + down).astype(BF16).astype(F32)
        gather(3, oall, i)
    arrived(3, oall)
    for p in range(n_sp):
        for i in range(parts_out):
            out_ref[:, p * co + i * cp:p * co + (i + 1) * cp] = oall[p, i].astype(BF16)
    for wait in sends:
        wait()
    rel_sent()


def solution(mesh):
    n_sp, n_tp = mesh.shape['sp'], mesh.shape['tp']
    spec_rows = P('dp', None)
    spec_cache = P('dp', 'sp', 'tp', None)
    in_specs = (spec_rows, spec_cache, spec_cache, P('dp'), P('sp', 'tp', None), P('tp', None), P('tp', None), P(None), P(None, 'tp', None), P(None, 'tp', None), P(None, 'tp', None), P('tp', None, None), P(None), P(None, 'tp'), P('tp', None))
    out_specs = spec_rows

    def layer_step(hidden, k_cache, v_cache, lengths, rel_table, u_bias, w_bias, g_attn, w_query, w_key, w_value, w_out, g_mlp, w_up, w_down):
        batch, seq_blk, heads, head_dim = k_cache.shape
        width = hidden.shape[1]
        ff = w_up.shape[1]
        rows = seq_blk * heads
        kk = width // n_sp
        co = width // n_sp
        rel_rows = rows // LANES
        vmem = functools.partial(pl.BlockSpec, memory_space=pltpu.VMEM)
        hbm = functools.partial(pl.BlockSpec, memory_space=pl.ANY)
        dma = pltpu.SemaphoreType.DMA
        phases = 4
        return pl.pallas_call(
            functools.partial(layer_kernel, n_sp, n_tp),
            out_shape=jax.ShapeDtypeStruct((batch, width), BF16),
            in_specs=[hbm()] * 15,
            out_specs=vmem(),
            scratch_shapes=[
                pltpu.SMEM((batch,), jnp.int32),
                pltpu.VMEM((batch, width), BF16),
                pltpu.VMEM((heads, head_dim), BF16),
                pltpu.VMEM((heads, head_dim), BF16),
                pltpu.VMEM((width,), BF16),
                pltpu.VMEM((width,), BF16),
                pltpu.VMEM((width * heads, head_dim), BF16),
                pltpu.VMEM((2, kk * heads, head_dim), BF16),
                pltpu.VMEM((width // LANES * batch, LANES), BF16),
                pltpu.VMEM((width // LANES * batch, LANES * heads), BF16),
                pltpu.VMEM((seq_blk, heads, head_dim), BF16),
                pltpu.VMEM((rows, head_dim), BF16),
                pltpu.VMEM((batch, rows, head_dim), BF16),
                pltpu.VMEM((batch, rows, head_dim), BF16),
                pltpu.VMEM((heads * head_dim, co), BF16),
                pltpu.VMEM((ff, co), BF16),
                pltpu.VMEM((n_sp, 2, batch, head_dim), F32),
                pltpu.VMEM((n_sp, 2, batch, head_dim), F32),
                pltpu.VMEM((n_sp, batch, head_dim), F32),
                pltpu.VMEM((batch, heads, head_dim), F32),
                pltpu.VMEM((batch, rel_rows, LANES), F32),
                *[pltpu.VMEM((batch // CHUNKS, (n_sp + 1) * rel_rows + 8, LANES), F32)] * CHUNKS,
                pltpu.VMEM((batch, rel_rows, LANES), F32),
                pltpu.VMEM((batch, 2 * heads, rows // 2), F32),
                pltpu.VMEM((CHUNKS, n_sp, 2 * batch // CHUNKS, head_dim), F32),
                pltpu.VMEM((CHUNKS, n_sp, 2 * batch // CHUNKS, head_dim), F32),
                pltpu.VMEM((n_sp, batch, head_dim), F32),
                pltpu.VMEM((OUT_PARTS, batch, co // OUT_PARTS), F32),
                pltpu.VMEM((OUT_PARTS, n_tp, batch, co // OUT_PARTS), F32),
                pltpu.VMEM((n_sp, OUT_PARTS, batch, co // OUT_PARTS), F32),
                pltpu.VMEM((UP_PARTS, batch, ff // UP_PARTS), F32),
                pltpu.VMEM((OUT_PARTS, batch, co // OUT_PARTS), F32),
                pltpu.VMEM((OUT_PARTS, n_tp, batch, co // OUT_PARTS), F32),
                pltpu.VMEM((n_sp, OUT_PARTS, batch, co // OUT_PARTS), F32),
                dma((19 + 3 * CHUNKS + UP_PARTS // CORES,)),
                dma((phases,)),
                dma((phases,)),
                dma((n_sp // CORES,)),
                dma((n_sp // CORES, CHUNKS)),
                dma((n_sp // CORES,)),
                dma((n_sp // CORES, CHUNKS)),
                dma((1,)),
                dma((1,)),
                dma((CHUNKS,)),
                dma((1,)),
                dma((1,)),
                dma((1,)),
                dma((1,)),
                dma((2, OUT_PARTS)),
                dma((2, OUT_PARTS)),
            ],
            compiler_params=pltpu.CompilerParams(collective_id=0, has_side_effects=True, vmem_limit_bytes=67043328),
            name='decode_layer',
        )(lengths, hidden, u_bias, w_bias, g_attn, g_mlp, rel_table,
          k_cache.reshape(batch, rows, head_dim), v_cache.reshape(batch, rows, head_dim),
          w_query.reshape(width * heads, head_dim), w_key.reshape(width * heads, head_dim), w_value.reshape(width * heads, head_dim),
          w_out.reshape(heads * head_dim, width), w_up, w_down)

    return jax.shard_map(layer_step, mesh=mesh, in_specs=in_specs, out_specs=out_specs, check_vma=False)
```

```python
import functools

import jax
import jax.numpy as jnp
from jax import lax
from jax.experimental import pallas as pl
from jax.experimental.pallas import tpu as pltpu
from jax.sharding import PartitionSpec as P

EPS = 1e-6
MASKED = -1e30
CORES = 2
CHUNKS = 4
UP_PARTS = 8
OUT_PARTS = 2
FLOOR = -5e29
LANES = 128
F32 = jnp.float32
BF16 = jnp.bfloat16
NT = (((1,), (1,)), ((), ()))


def layer_kernel(n_sp, n_tp,
                 lens_in, hid_in, u_in, w_in, ga_in, gm_in, rel_hbm, k_hbm, v_hbm, wq_hbm, wk_hbm, wv_hbm, wo_hbm, wu_hbm, wd_hbm,
                 out_ref,
                 lens, hid, u_ref, w_ref, ga, gm,
                 wqb, wkvb, normed, spread_x, relb, rrev, kb, vb, wob, wdb,
                 kvsend, kvrecv, qall, qcb, relsend, grid_rel0, grid_rel1, grid_rel2, grid_rel3, win, sc, csend, crecv, call, aosend, aorecv,
                 x1all, aall, dnsend, dnrecv, oall,
                 hsem, ssem, rsem, rel_ssem, rel_rsem, fwd_ssem, fwd_rsem, relay_ssem, sib_ssem, sib_rsem, ctx_ssem, ctx_rsem, a_ssem, a_rsem, tp_ssem, tp_rsem):
    me = lax.axis_index('sp')
    my_tp = lax.axis_index('tp')
    batch = hid.shape[0]
    heads = u_ref.shape[0]
    head_dim = u_ref.shape[1]
    rows = kb.shape[1]
    seq_blk = rows // heads
    kk = wkvb.shape[1] // heads
    pieces = 8
    chunks = CHUNKS
    chunk = batch // chunks
    chips = n_sp // CORES
    chip, core = me // CORES, me % CORES
    sibling = chip * CORES + 1 - core
    co = wob.shape[1]
    per_row = LANES // heads
    rel_rows = seq_blk // per_row
    smax = seq_blk * n_sp
    half = rows // 2
    half_ff = wu_hbm.shape[1] // CORES
    scale = head_dim ** -0.5

    grid_rel = (grid_rel0, grid_rel1, grid_rel2, grid_rel3)
    copies = []

    def fetch(src, dst, sem=None):
        copy = pltpu.make_async_copy(src, dst, hsem.at[len(copies) if sem is None else sem])
        if sem is None:
            copies.append(copy)
        copy.start()
        return copy

    small = [fetch(hid_in, hid), fetch(ga_in, ga), fetch(u_in, u_ref), fetch(w_in, w_ref), fetch(gm_in, gm), fetch(lens_in, lens)]
    rel_copy = fetch(rel_hbm, relb)
    first_q = len(copies)
    piece = wqb.shape[0] // pieces
    q_copies = [fetch(wq_hbm.at[i * piece:(i + 1) * piece], wqb.at[i * piece:(i + 1) * piece]) for i in range(pieces)]
    w_rows = pl.ds(pl.multiple_of(me * kk * heads, kk * heads), kk * heads)
    w_copies = [fetch(src.at[w_rows], wkvb.at[i]) for i, src in enumerate((wk_hbm, wv_hbm))]
    k_copies = [fetch(k_hbm.at[g * chunk:(g + 1) * chunk], kb.at[g * chunk:(g + 1) * chunk]) for g in range(chunks)]
    v_copies = [fetch(v_hbm.at[g * chunk:(g + 1) * chunk], vb.at[g * chunk:(g + 1) * chunk]) for g in range(chunks)]
    o_cols = pl.ds(pl.multiple_of(me * co, co), co)
    wo_copy = fetch(wo_hbm.at[:, o_cols], wob)
    wd_copy = fetch(wd_hbm.at[:, o_cols], wdb)

    peers = [(lax.rem(chip + dx, chips) * CORES + (core if e == 0 else 1 - core))
             for dx in sorted(range(chips), key=lambda d: -min(d, chips - d)) for e in range(CORES) if (dx, e) != (0, 0)]

    def tp_peer(off):
        return lax.rem(my_tp + off, n_tp)

    for part in grid_rel:
        part[...] = jnp.zeros_like(part)

    barrier = pltpu.get_barrier_semaphore()
    for peer in peers:
        pl.semaphore_signal(barrier, inc=1, device_id={'sp': peer}, device_id_type=pl.DeviceIdType.MESH)
    for off in range(1, n_tp):
        pl.semaphore_signal(barrier, inc=1, device_id={'tp': tp_peer(off)}, device_id_type=pl.DeviceIdType.MESH)

    def remote(src, dst, send, recv, where):
        return pltpu.make_async_remote_copy(src_ref=src, dst_ref=dst, send_sem=send, recv_sem=recv, device_id=where,
                                            device_id_type=pl.DeviceIdType.MESH)

    sends = []

    def later(src, sem):
        sends.append(lambda: remote(src, src, sem, sem, {'sp': sibling}).wait_send())

    def take(dst, sem):
        remote(dst, dst, sem, sem, {'sp': sibling}).wait_recv()

    others = slice(0, n_sp - 1)

    def scatter(phase, src, dst):
        for peer in peers:
            remote(src.at[peer], dst.at[me], ssem.at[phase], rsem.at[phase], {'sp': peer}).start()
        later(src.at[others], ssem.at[phase])

    def gather(phase, buf, part=None):
        block = buf.at[me] if part is None else buf.at[me, part]
        for peer in peers:
            remote(block, block, ssem.at[phase], rsem.at[phase], {'sp': peer}).start()
        if part is None or part == buf.shape[1] - 1:
            later(buf.at[others], ssem.at[phase])

    def arrived(phase, buf):
        take(buf.at[others], rsem.at[phase])

    def tp_send(phase, part, src, dst):
        dst[part, my_tp] = src[part]
        for off in sorted(range(1, n_tp), key=lambda d: -min(d, n_tp - d)):
            remote(src.at[part], dst.at[part, my_tp], tp_ssem.at[phase, part], tp_rsem.at[phase, part], {'tp': tp_peer(off)}).start()
        later(dst.at[part, 0:n_tp - 1], tp_ssem.at[phase, part])

    def tp_total(phase, part, dst):
        take(dst.at[part, 0:n_tp - 1], tp_rsem.at[phase, part])
        total = dst[part, 0]
        for t in range(1, n_tp):
            total = total + dst[part, t]
        return total

    for copy in small:
        copy.wait()
    wide = hid[...].astype(F32)
    inv = lax.rsqrt(jnp.mean(wide * wide, axis=-1, keepdims=True) + EPS)
    whole = (wide * inv * ga[...].reshape(1, wide.shape[1]).astype(F32)).astype(BF16)
    n_in = wide.shape[1] // LANES
    for c in range(n_in):
        normed[c * batch:(c + 1) * batch] = whole[:, c * LANES:(c + 1) * LANES]
    span = LANES * heads
    spread = (lax.broadcasted_iota(jnp.int32, (LANES, span), 1) // heads
              == lax.broadcasted_iota(jnp.int32, (LANES, span), 0)).astype(F32).astype(BF16)
    lane_head = lax.broadcasted_iota(jnp.int32, (batch, LANES), 1) % heads
    head_mask = [jnp.concatenate([(lane_head == h).astype(F32).astype(BF16)] * heads, axis=1) for h in range(heads)]

    spread_x[...] = jnp.dot(normed[...], spread, preferred_element_type=F32).astype(BF16)

    def by_head(c):
        spread_in = spread_x[pl.ds(pl.multiple_of(c * batch, batch), batch), :]
        return jnp.concatenate([spread_in * head_mask[h] for h in range(heads)], axis=0)

    rel_copy.wait()
    group = 32

    def reverse(i, carry):
        tile = relb[pl.ds(pl.multiple_of(i * group, group), group)].astype(F32)
        flipped = jnp.concatenate([tile[group - 1 - j:group - j] for j in range(group)], axis=0)
        flipped = flipped.reshape(group * heads, head_dim).astype(BF16)
        at = pl.multiple_of((seq_blk // group - 1 - i) * group * heads, group * heads)
        rrev[pl.ds(at, group * heads), :] = flipped
        return carry

    lax.fori_loop(0, seq_blk // group, reverse, 0)

    def project(i, acc):
        pltpu.make_async_copy(wq_hbm.at[pl.ds(0, piece)], wqb.at[pl.ds(0, piece)], hsem.at[first_q + i]).wait()
        per = piece // span
        for j in range(per):
            at = pl.multiple_of((i * per + j) * span, span)
            acc = acc + jnp.dot(by_head(i * per + j), wqb[pl.ds(at, span), :], preferred_element_type=F32)
        return acc

    acc = lax.fori_loop(0, pieces, project, jnp.zeros((heads * batch, head_dim), F32))
    for h in range(heads):
        qall[h] = acc[h * batch:(h + 1) * batch].astype(BF16).astype(F32)

    u_wide, w_wide = u_ref[...].astype(F32), w_ref[...].astype(F32)
    q_pos = jnp.concatenate([(qall[h] + w_wide[h:h + 1]).astype(BF16) for h in range(heads)], axis=0)

    def relative(c, carry):
        tiles_now = 4
        wide_span = tiles_now * LANES
        table = rrev[c * wide_span:(c + 1) * wide_span, :]
        scores = lax.dot_general(q_pos, table, NT, preferred_element_type=F32)
        for t in range(tiles_now):
            tile = scores[:, t * LANES:(t + 1) * LANES]
            row = tile[:batch]
            for h in range(1, heads):
                row = jnp.where(lane_head == h, tile[h * batch:(h + 1) * batch], row)
            at = tiles_now * c + t
            relsend[:, at:at + 1, :] = row.reshape(batch, 1, LANES)
        return carry

    for c in range(rows // (4 * LANES)):
        relative(c, 0)

    half_rows = rel_rows // CORES

    def seqs(g):
        return pl.ds(g * chunk, chunk)

    def spot(src, to_chip, g, first, size):
        at = (n_sp - 1 - src - CORES * to_chip) * rel_rows + first
        return grid_rel[g].at[:, pl.ds(pl.multiple_of(at, half_rows), size), :]

    def needed(a, b):
        return a + b <= chips - 1

    def rel_out(dx, parts):
        to_chip = lax.rem(chip + dx, chips)

        @pl.when(needed(to_chip, chip))
        def _():
            for g in range(chunks):
                for part in parts:
                    remote(relsend.at[seqs(g), part * half_rows:(part + 1) * half_rows, :],
                           spot(me, to_chip, g, part * half_rows, half_rows),
                           rel_ssem.at[dx], rel_rsem.at[chip, g], {'sp': to_chip * CORES + part}).start()

    def rel_out_first():
        rel_out(chips - 1, (1,))
        rel_out(chips // 2, (0,))
        for dx in range(1, chips - 1):
            if 2 * dx != chips:
                rel_out(dx, (0, 1))

        @pl.when(needed(chip, chip))
        def _():
            for g in range(chunks):
                remote(relsend.at[seqs(g)], spot(me, chip, g, 0, rel_rows), sib_ssem.at[0], sib_rsem.at[g], {'sp': sibling}).start()

    def each_source(fn):
        for dx in range(1, chips):
            from_chip = lax.rem(chip + dx, chips)

            @pl.when(needed(from_chip, chip))
            def _():
                fn(dx, from_chip)

    def pass_on(g, dx, from_chip, c, act):
        src = from_chip * CORES + c
        mine = spot(src, chip, g, core * half_rows, half_rows)
        act(remote(mine, mine, fwd_ssem.at[dx], fwd_rsem.at[from_chip, g], {'sp': sibling}))
        if dx == 1:
            to_chip = lax.rem(chip + chips - 1, chips)

            @pl.when(jnp.logical_and(core == 1, needed(to_chip, from_chip)))
            def _():
                act(remote(mine, spot(src, to_chip, g, half_rows, half_rows), relay_ssem.at[0], rel_rsem.at[from_chip, g],
                           {'sp': to_chip * CORES + 1}))

    both = relsend.at[0:chunk]

    def source_in(g, dx):
        from_chip = lax.rem(chip + dx, chips)

        @pl.when(needed(from_chip, chip))
        def _():
            take(both, rel_rsem.at[from_chip, g])
            for c in range(CORES):
                pass_on(g, dx, from_chip, c, lambda copy: copy.start())

    def rel_in_first():
        @pl.when(core == 1)
        def _():
            for g in range(chunks):
                source_in(g, 1)

    def rel_in(g):
        @pl.when(core == 0)
        def _():
            source_in(g, 1)

        for dx in range(2, chips):
            source_in(g, dx)

    def rel_done(g):
        each_source(lambda dx, from_chip: take(both, fwd_rsem.at[from_chip, g]))

        @pl.when(needed(chip, chip))
        def _():
            take(both, sib_rsem.at[g])

    def rel_sent():
        for dx in range(1, chips):
            to_chip = lax.rem(chip + dx, chips)
            sent = relsend.at[:, 0:half_rows] if 2 * dx == chips else relsend

            @pl.when(needed(to_chip, chip))
            def _():
                remote(sent, sent, rel_ssem.at[dx], rel_ssem.at[dx], {'sp': sibling}).wait_send()
                remote(relsend, relsend, fwd_ssem.at[dx], fwd_ssem.at[dx], {'sp': sibling}).wait_send()

        @pl.when(needed(chip, chip))
        def _():
            remote(relsend, relsend, sib_ssem.at[0], sib_ssem.at[0], {'sp': sibling}).wait_send()

        to_chip, from_chip = lax.rem(chip + chips - 1, chips), lax.rem(chip + 1, chips)

        @pl.when(jnp.logical_and(jnp.logical_and(core == 1, needed(from_chip, chip)), needed(to_chip, from_chip)))
        def _():
            remote(relsend, relsend, relay_ssem.at[0], relay_ssem.at[0], {'sp': sibling}).wait_send()

    pl.semaphore_wait(barrier, n_sp + n_tp - 2)
    rel_out_first()

    @pl.when(needed(chip, chip))
    def _():
        at = pl.multiple_of((n_sp - 1 - me - CORES * chip) * rel_rows, rel_rows)
        for g in range(chunks):
            grid_rel[g][:, pl.ds(at, rel_rows), :] = relsend[seqs(g)]

    for i in range(2):
        w_copies[i].wait()
    lhs_first = me * (kk // LANES)
    acc = [jnp.zeros((heads * batch, head_dim), F32)] * 2
    for c in range(kk // LANES):
        lhs = by_head(lhs_first + c)
        acc = [acc[i] + jnp.dot(lhs, wkvb[i, c * span:(c + 1) * span, :], preferred_element_type=F32) for i in range(2)]
    for i in range(2):
        for h in range(heads):
            kvsend[h, i] = acc[i][h * batch:(h + 1) * batch]
    scatter(0, kvsend, kvrecv)
    kvrecv[me] = kvsend[me]

    for h in range(heads):
        qcb[:, h:h + 1, :] = (qall[h] + u_wide[h:h + 1]).reshape(batch, 1, head_dim)

    def content_of(g):
        k_copies[g].wait()
        for j in range(chunk):
            b = g * chunk + j
            q = qcb[b]
            zero = jnp.zeros_like(q)
            two = jnp.concatenate([jnp.concatenate([q, zero], axis=1), jnp.concatenate([zero, q], axis=1)], axis=0).astype(BF16)
            for c in range(half // 256):
                keys = jnp.concatenate([kb[b, c * 256:(c + 1) * 256, :], kb[b, half + c * 256:half + (c + 1) * 256, :]], axis=1)
                sc[b, :, c * 256:(c + 1) * 256] = lax.dot_general(two, keys, NT, preferred_element_type=F32)

    r_iota = lax.broadcasted_iota(jnp.int32, (2 * heads, LANES), 0)
    l_iota = lax.broadcasted_iota(jnp.int32, (2 * heads, LANES), 1)
    slot = me * seq_blk + (r_iota // heads) * (seq_blk // 2) + l_iota // heads
    slot = jnp.where(r_iota % heads == l_iota % heads, slot, jnp.int32(2 ** 30))
    lane_row = lax.broadcasted_iota(jnp.int32, (rel_rows, LANES), 1)
    first_stat = lax.broadcasted_iota(jnp.int32, (heads, LANES), 1) < LANES // 2
    tiles = half // LANES

    def attend(g, j):
        b = g * chunk + j
        n = lens[b]
        start = smax - 1 - n
        row0 = jnp.minimum(start // per_row + core * rel_rows, n_sp * rel_rows - 1)
        turn = LANES - heads * (start % per_row)
        now = pltpu.roll(grid_rel[g][j, pl.ds(row0, rel_rows), :], turn, 1)
        after = pltpu.roll(grid_rel[g][j, pl.ds(row0 + 1, rel_rows), :], turn, 1)
        win[b] = jnp.where(lane_row < turn, now, after)
        scores = []
        for c in range(tiles):
            rel = jnp.concatenate([jnp.broadcast_to(win[b, c:c + 1, :], (heads, LANES)),
                                   jnp.broadcast_to(win[b, tiles + c:tiles + c + 1, :], (heads, LANES))], axis=0)
            s = (sc[b, :, c * LANES:(c + 1) * LANES] + rel) * scale
            scores.append(jnp.where(slot < n - c * per_row, s, MASKED))
        top = functools.reduce(jnp.maximum, scores)
        top = jnp.max(top, axis=1, keepdims=True)
        top = jnp.maximum(jnp.maximum(top[:heads], top[heads:]), FLOOR)
        top2 = jnp.concatenate([top, top], axis=0)
        weights = [jnp.exp(s - top2) for s in scores]
        total = jnp.sum(functools.reduce(jnp.add, weights), axis=1, keepdims=True)
        total = total[:heads] + total[heads:]
        acc = jnp.zeros((2 * heads, 2 * head_dim), F32)
        for c in range(half // 256):
            values = jnp.concatenate([vb[b, c * 256:(c + 1) * 256, :], vb[b, half + c * 256:half + (c + 1) * 256, :]], axis=1)
            p = jnp.concatenate([weights[2 * c], weights[2 * c + 1]], axis=1).astype(BF16)
            acc = acc + jnp.dot(p, values, preferred_element_type=F32)
        ctx = acc[:heads, :head_dim] + acc[heads:, head_dim:]
        csend[g, :, j:j + 1, :] = ctx.reshape(heads, 1, head_dim)
        stats = jnp.where(first_stat, top, total)
        csend[g, :, chunk + j:chunk + j + 1, :] = stats.reshape(heads, 1, LANES)

    def attend_of(g):
        for j in range(chunk):
            attend(g, j)
        for peer in peers:
            remote(csend.at[g, peer], crecv.at[g, me], ctx_ssem.at[0], ctx_rsem.at[0], {'sp': peer}).start()
        crecv[g, me] = csend[g, me]

    content_of(0)
    rel_out(chips - 1, (0,))
    content_of(1)
    content_of(2)
    rel_in_first()
    content_of(3)
    up_cols = half_ff // batch
    first_up = len(copies)
    up_groups = aall.shape[0] // CORES
    for t in range(batch):
        fetch(wu_hbm.at[:, pl.ds(pl.multiple_of(core * half_ff + t * up_cols, up_cols), up_cols)], kb.at[t],
              first_up + t // (batch // up_groups))
    rel_in(0)
    rel_in(1)
    for g in range(chunks):
        if 0 < g < chunks - 1:
            rel_in(g + 1)
        rel_done(g)
        v_copies[g].wait()
        attend_of(g)

    arrived(0, kvrecv)
    k_new, v_new = kvrecv[0, 0], kvrecv[0, 1]
    for p in range(1, n_sp):
        k_new, v_new = k_new + kvrecv[p, 0], v_new + kvrecv[p, 1]
    k_new = k_new.astype(BF16).astype(F32)
    v_new = v_new.astype(BF16).astype(F32)
    q_cont = (qall[me] + jnp.sum(jnp.where(lax.broadcasted_iota(jnp.int32, (heads, head_dim), 0) == me, u_wide, 0.0), axis=0, keepdims=True))
    q_cont = q_cont.astype(BF16).astype(F32)
    last_row = (n_sp - 1 - CORES * chip) * rel_rows + rel_rows - 1
    zero_dist = jnp.concatenate([part[:, pl.ds(last_row, 1), :].reshape(chunk, LANES) for part in grid_rel], axis=0)
    lane_b = lax.broadcasted_iota(jnp.int32, (batch, LANES), 1)
    rel0 = jnp.sum(jnp.where(lane_b == LANES - heads + me, zero_dist, 0.0), axis=1, keepdims=True)
    s_new = (jnp.sum(q_cont * k_new, axis=1, keepdims=True) + rel0) * scale

    later(csend.at[:, others], ctx_ssem.at[0])
    take(crecv.at[:, others], ctx_rsem.at[0])
    parts = [jnp.concatenate([crecv[g, p, :chunk] for g in range(chunks)], axis=0) for p in range(n_sp)]
    stats = [jnp.concatenate([crecv[g, p, chunk:] for g in range(chunks)], axis=0) for p in range(n_sp)]
    tops = [t[:, :1] for t in stats]
    sums = [t[:, LANES - 1:] for t in stats]
    best = functools.reduce(jnp.maximum, tops, s_new)
    e_new = jnp.exp(s_new - best)
    denom = e_new
    numer = e_new.astype(BF16).astype(F32) * v_new
    for p in range(n_sp):
        factor = jnp.exp(tops[p] - best)
        denom = denom + factor * sums[p]
        numer = numer + factor * parts[p]
    call[me] = (numer / denom).astype(BF16).astype(F32)
    gather(1, call)
    arrived(1, call)

    ctx_all = jnp.concatenate([call[h].astype(BF16) for h in range(heads)], axis=1)
    wo_copy.wait()
    parts_out, cp = aosend.shape[0], aosend.shape[2]
    attn_part = jnp.dot(ctx_all, wob[...], preferred_element_type=F32)
    for i in range(parts_out):
        aosend[i] = attn_part[:, i * cp:(i + 1) * cp]
        tp_send(0, i, aosend, aorecv)
    for i in range(parts_out):
        attn = tp_total(0, i, aorecv)
        x1_cols = pl.ds(pl.multiple_of(me * co + i * cp, cp), cp)
        x1all[me, i] = (hid[:, x1_cols].astype(F32) + attn).astype(BF16).astype(F32)
        gather(2, x1all, i)
    arrived(2, x1all)
    x1_parts = [x1all[p, i] for p in range(n_sp) for i in range(parts_out)]
    mean_sq = functools.reduce(jnp.add, [jnp.sum(t * t, axis=-1, keepdims=True) for t in x1_parts]) / (co * n_sp)
    inv = lax.rsqrt(mean_sq + EPS)
    gain = gm[...].reshape(1, co * n_sp).astype(F32)
    normed_mid = jnp.concatenate([(t * inv * gain[:, p * cp:(p + 1) * cp]).astype(BF16) for p, t in enumerate(x1_parts)], axis=1)
    per_part = aall.shape[2] // up_cols
    for i in range(aall.shape[0] // CORES):
        tiles_up = kb.at[i * per_part:(i + 1) * per_part]
        pltpu.make_async_copy(tiles_up, tiles_up, hsem.at[first_up + i]).wait()
        at = core * (aall.shape[0] // CORES) + i
        weights = jnp.concatenate([kb[t] for t in range(i * per_part, (i + 1) * per_part)], axis=1)
        up = jnp.dot(normed_mid, weights, preferred_element_type=F32)
        aall[at] = jax.nn.gelu(up, approximate=True).astype(BF16).astype(F32)
        remote(aall.at[at], aall.at[at], a_ssem.at[0], a_rsem.at[0], {'sp': sibling}).start()
    later(aall.at[0:up_groups], a_ssem.at[0])

    def down_of(which):
        act = jnp.concatenate([aall[which * up_groups + i].astype(BF16) for i in range(up_groups)], axis=1)
        units = pl.ds(pl.multiple_of(which * half_ff, half_ff), half_ff)
        return jnp.dot(act, wdb[units, :], preferred_element_type=F32)

    wd_copy.wait()
    down_part = down_of(core)
    take(aall.at[0:up_groups], a_rsem.at[0])
    down_part = down_part + down_of(1 - core)
    for i in range(parts_out):
        dnsend[i] = down_part[:, i * cp:(i + 1) * cp]
        tp_send(1, i, dnsend, dnrecv)
    for i in range(parts_out):
        down = tp_total(1, i, dnrecv)
        oall[me, i] = (x1all[me, i] + down).astype(BF16).astype(F32)
        gather(3, oall, i)
    arrived(3, oall)
    for p in range(n_sp):
        for i in range(parts_out):
            out_ref[:, p * co + i * cp:p * co + (i + 1) * cp] = oall[p, i].astype(BF16)
    for wait in sends:
        wait()
    rel_sent()


def solution(mesh):
    n_sp, n_tp = mesh.shape['sp'], mesh.shape['tp']
    spec_rows = P('dp', None)
    spec_cache = P('dp', 'sp', 'tp', None)
    in_specs = (spec_rows, spec_cache, spec_cache, P('dp'), P('sp', 'tp', None), P('tp', None), P('tp', None), P(None), P(None, 'tp', None), P(None, 'tp', None), P(None, 'tp', None), P('tp', None, None), P(None), P(None, 'tp'), P('tp', None))
    out_specs = spec_rows

    def layer_step(hidden, k_cache, v_cache, lengths, rel_table, u_bias, w_bias, g_attn, w_query, w_key, w_value, w_out, g_mlp, w_up, w_down):
        batch, seq_blk, heads, head_dim = k_cache.shape
        width = hidden.shape[1]
        ff = w_up.shape[1]
        rows = seq_blk * heads
        kk = width // n_sp
        co = width // n_sp
        rel_rows = rows // LANES
        vmem = functools.partial(pl.BlockSpec, memory_space=pltpu.VMEM)
        hbm = functools.partial(pl.BlockSpec, memory_space=pl.ANY)
        dma = pltpu.SemaphoreType.DMA
        phases = 4
        return pl.pallas_call(
            functools.partial(layer_kernel, n_sp, n_tp),
            out_shape=jax.ShapeDtypeStruct((batch, width), BF16),
            in_specs=[hbm()] * 15,
            out_specs=vmem(),
            scratch_shapes=[
                pltpu.SMEM((batch,), jnp.int32),
                pltpu.VMEM((batch, width), BF16),
                pltpu.VMEM((heads, head_dim), BF16),
                pltpu.VMEM((heads, head_dim), BF16),
                pltpu.VMEM((width,), BF16),
                pltpu.VMEM((width,), BF16),
                pltpu.VMEM((width * heads, head_dim), BF16),
                pltpu.VMEM((2, kk * heads, head_dim), BF16),
                pltpu.VMEM((width // LANES * batch, LANES), BF16),
                pltpu.VMEM((width // LANES * batch, LANES * heads), BF16),
                pltpu.VMEM((seq_blk, heads, head_dim), BF16),
                pltpu.VMEM((rows, head_dim), BF16),
                pltpu.VMEM((batch, rows, head_dim), BF16),
                pltpu.VMEM((batch, rows, head_dim), BF16),
                pltpu.VMEM((heads * head_dim, co), BF16),
                pltpu.VMEM((ff, co), BF16),
                pltpu.VMEM((n_sp, 2, batch, head_dim), F32),
                pltpu.VMEM((n_sp, 2, batch, head_dim), F32),
                pltpu.VMEM((n_sp, batch, head_dim), F32),
                pltpu.VMEM((batch, heads, head_dim), F32),
                pltpu.VMEM((batch, rel_rows, LANES), F32),
                *[pltpu.VMEM((batch // CHUNKS, (n_sp + 1) * rel_rows + 8, LANES), F32)] * CHUNKS,
                pltpu.VMEM((batch, rel_rows, LANES), F32),
                pltpu.VMEM((batch, 2 * heads, rows // 2), F32),
                pltpu.VMEM((CHUNKS, n_sp, 2 * batch // CHUNKS, head_dim), F32),
                pltpu.VMEM((CHUNKS, n_sp, 2 * batch // CHUNKS, head_dim), F32),
                pltpu.VMEM((n_sp, batch, head_dim), F32),
                pltpu.VMEM((OUT_PARTS, batch, co // OUT_PARTS), F32),
                pltpu.VMEM((OUT_PARTS, n_tp, batch, co // OUT_PARTS), F32),
                pltpu.VMEM((n_sp, OUT_PARTS, batch, co // OUT_PARTS), F32),
                pltpu.VMEM((UP_PARTS, batch, ff // UP_PARTS), F32),
                pltpu.VMEM((OUT_PARTS, batch, co // OUT_PARTS), F32),
                pltpu.VMEM((OUT_PARTS, n_tp, batch, co // OUT_PARTS), F32),
                pltpu.VMEM((n_sp, OUT_PARTS, batch, co // OUT_PARTS), F32),
                dma((19 + 3 * CHUNKS + UP_PARTS // CORES,)),
                dma((phases,)),
                dma((phases,)),
                dma((n_sp // CORES,)),
                dma((n_sp // CORES, CHUNKS)),
                dma((n_sp // CORES,)),
                dma((n_sp // CORES, CHUNKS)),
                dma((1,)),
                dma((1,)),
                dma((CHUNKS,)),
                dma((1,)),
                dma((1,)),
                dma((1,)),
                dma((1,)),
                dma((2, OUT_PARTS)),
                dma((2, OUT_PARTS)),
            ],
            compiler_params=pltpu.CompilerParams(collective_id=0, has_side_effects=True, vmem_limit_bytes=67043328),
            name='decode_layer',
        )(lengths, hidden, u_bias, w_bias, g_attn, g_mlp, rel_table,
          k_cache.reshape(batch, rows, head_dim), v_cache.reshape(batch, rows, head_dim),
          w_query.reshape(width * heads, head_dim), w_key.reshape(width * heads, head_dim), w_value.reshape(width * heads, head_dim),
          w_out.reshape(heads * head_dim, width), w_up, w_down)

    return jax.shard_map(layer_step, mesh=mesh, in_specs=in_specs, out_specs=out_specs, check_vma=False)
```
